32 devices in a mesh: dp: 4 (over x, core), ctx: 8 (over z, y).
Axes of the slice: x: 2, y: 2, z: 4, core: 2. Of those that a mesh axis runs over, the one named last changes fastest.
Arguments:
- frames: bfloat16 [4, 40, 16, 16, 512], P('dp', 'ctx'), may hold values from -6 to 6
- stream: bfloat16 [4, 40, 64, 3072], P('dp', 'ctx'), may hold values from -6 to 6
- video_frames: int32 [4], P('dp'), may hold values from 1 to 40
- conv_weight: bfloat16 [3, 3, 3, 512, 512], replicated, may hold values from -0.0546875 to 0.0546875
- latent_weight: bfloat16 [512, 16], replicated, may hold values from -0.25 to 0.25
- embed_weight: bfloat16 [64, 3072], replicated, may hold values from -0.75 to 0.75
- norm_gain: float32 [3072], replicated, may hold values from 0.25 to 1.75
- qkv_weight: bfloat16 [3072, 4608], P('ctx', 'dp'), may hold values from -0.109375 to 0.109375
Outputs:
- section: bfloat16 [4, 40, 16, 16, 512], P('dp', 'ctx')
- mixed: bfloat16 [4, 40, 64, 1536], P('dp', 'ctx')
The draws below stay inside these ranges and needn't reach their ends.
All inputs are finite; a program needn't handle non-finite values.
Results may differ from the reference program's by a relative error of at most 0.0061.
Values may be sent and summed in bfloat16 or wider, within the bound.
No kernel may reach another device: no remote copies, remote signals or barrier semaphores. Data moves between devices by JAX's collectives and lax.ppermute only.
A program may use at most 128 MiB of HBM per device.

```python
import jax
import jax.numpy as jnp
from jax import lax

CH = 512
LAT = 16
D = 3072
HEADS = 12
HD = 128
HT = 16
WT = 16
NF = 40
GROUPS = 4
TOKF = 64


def with_ends(entries, rng, least, largest):
    shape = entries.shape
    spot = [jax.random.randint(jax.random.fold_in(rng, axis), (), 0, shape[axis]) for axis in range(len(shape))]
    entries = entries.at[tuple(spot)].set(least)
    longest = shape.index(max(shape))
    spot[longest] = (spot[longest] + 1) % shape[longest]
    return entries.at[tuple(spot)].set(largest)


def block_scale(rng, extent, pieces, low, top_value):
    def one(position, blocks):
        heights = jax.random.uniform(jax.random.fold_in(jax.random.fold_in(rng, 6), position), (blocks,), jnp.float32, low / len(pieces), top_value / len(pieces))
        return jnp.repeat(jnp.exp(heights), extent[position] // blocks).reshape((-1,) + (1,) * (len(extent) - position - 1))

    gain = one(*pieces[0])
    for cut in pieces[1:]:
        gain = gain * one(*cut)
    return gain


def gaussian(own_key, dims, deviation, most, cuts=(), held_as=jnp.bfloat16):
    factor_of = block_scale(own_key, dims, cuts, -0.22, 0.18) if cuts else 1.0
    values = jax.random.normal(own_key, dims, jnp.float32) * deviation * factor_of
    return jnp.minimum(jnp.maximum(values, -most), most).astype(held_as)


def setup_inputs(seed: int = 0) -> dict:
    seeds = jax.random.split(jax.random.key(seed), 9)
    frames = gaussian(seeds[0], (GROUPS, NF, HT, WT, CH), 1.0, 6.0, ((0, 4), (1, 8)))
    stream = gaussian(seeds[1], (GROUPS, NF, TOKF, D), 1.0, 6.0, ((0, 4), (1, 8)))
    video_frames = with_ends(jax.random.randint(seeds[2], (GROUPS,), 1, NF + 1), jax.random.fold_in(seeds[2], 1), 1, NF).astype(jnp.int32)
    conv_weight = gaussian(seeds[3], (3, 3, 3, CH, CH), (27 * CH) ** -0.5, 0.0546875)
    latent_weight = gaussian(seeds[4], (CH, LAT), CH ** -0.5, 0.25)
    embed_weight = gaussian(seeds[5], (4 * LAT, D), (4 * LAT) ** -0.5, 0.75)
    norm_gain = jnp.clip(1.0 + 0.15 * jax.random.normal(seeds[6], (D,), jnp.float32), 0.25, 1.75)
    qkv_weight = gaussian(seeds[7], (D, 3 * HEADS * HD), D ** -0.5, 0.109375, ((0, 8), (1, 4)))
    return dict(frames=frames, stream=stream, video_frames=video_frames, conv_weight=conv_weight, latent_weight=latent_weight, embed_weight=embed_weight, norm_gain=norm_gain, qkv_weight=qkv_weight)


def conv_group(args):
    act_group, length, conv_weight = args
    padded = jnp.pad(act_group, ((2, 0), (1, 1), (1, 1), (0, 0)))
    frame_ids = jnp.arange(NF, dtype=jnp.int32)
    total = jnp.zeros((NF * HT * WT, CH), jnp.float32)
    for lag in range(3):
        part = jnp.zeros((NF * HT * WT, CH), jnp.float32)
        for row in range(3):
            for col in range(3):
                slab = padded[2 - lag:2 - lag + NF, row:row + HT, col:col + WT, :].reshape(-1, CH)
                part = part + jnp.dot(slab, conv_weight[lag, row, col], preferred_element_type=jnp.float32)
        if lag == 0:
            total = total + part
        else:
            valid = ((frame_ids < length) & (frame_ids >= lag)).astype(jnp.float32)
            total = total + part * jnp.repeat(valid, HT * WT)[:, None]
    return total

def attend_group(args):
    block, length = args
    query = block[..., 0:HD].astype(jnp.float32)
    keys = block[..., HD:2 * HD].astype(jnp.float32)
    values = block[..., 2 * HD:3 * HD].astype(jnp.float32)
    scores = jnp.einsum('tphd,sphd->phts', query, keys, precision=lax.Precision.HIGHEST) * HD ** (-0.5)
    frame_ids = jnp.arange(NF, dtype=jnp.int32)
    video = frame_ids < length
    allowed = video[:, None] & video[None, :] | (frame_ids[:, None] == frame_ids[None, :])
    scores = jnp.where(allowed, scores, -1e+30)
    top = lax.optimization_barrier(jnp.max(scores, axis=-1, keepdims=True))
    expo = jnp.exp(scores - top)
    probs = (expo / lax.optimization_barrier(jnp.sum(expo, axis=-1, keepdims=True))).astype(jnp.bfloat16)
    out = jnp.einsum('phts,sphd->tphd', probs.astype(jnp.float32), values, precision=lax.Precision.HIGHEST)
    return out.astype(jnp.bfloat16)

def reference(frames, stream, video_frames, conv_weight, latent_weight, embed_weight, norm_gain, qkv_weight):
    act = jax.nn.silu(frames.astype(jnp.float32)).astype(jnp.bfloat16)
    conv = lax.map(lambda pair: conv_group((pair[0], pair[1], conv_weight)), (act, video_frames))
    section = (frames.astype(jnp.float32) + conv.reshape(frames.shape)).astype(jnp.bfloat16)
    latent = jnp.dot(section.reshape(-1, CH), latent_weight, preferred_element_type=jnp.float32).astype(jnp.bfloat16)
    latent = latent.reshape(GROUPS, NF, HT // 2, 2, WT // 2, 2, LAT).transpose(0, 1, 2, 4, 3, 5, 6)
    patches = latent.reshape(-1, 4 * LAT)
    embedded = jnp.dot(patches, embed_weight, preferred_element_type=jnp.float32) + stream.reshape(-1, D).astype(jnp.float32)
    scale = lax.rsqrt(lax.optimization_barrier(jnp.mean(embedded * embedded, axis=-1, keepdims=True)) + 1e-06)
    normed = (embedded * scale * norm_gain).astype(jnp.bfloat16)
    qkv = jnp.dot(normed, qkv_weight, preferred_element_type=jnp.float32).astype(jnp.bfloat16)
    qkv = qkv.reshape(GROUPS, NF, TOKF, HEADS, 3 * HD)
    mixed = lax.map(attend_group, (qkv, video_frames))
    return (section, mixed.reshape(GROUPS, NF, TOKF, HEADS * HD))
```

```python
import jax
import jax.numpy as jnp
from jax import lax
from jax.sharding import PartitionSpec as P

HD = 128


def rotate(value, axis, steps):
    count = lax.axis_size(axis)
    steps = steps % count
    if steps == 0:
        return value
    return lax.ppermute(value, axis, [(i, (i + steps) % count) for i in range(count)])


def flip(value, axis, bit):
    count = lax.axis_size(axis)
    return lax.ppermute(value, axis, [(i, i ^ bit) for i in range(count)])


def butterfly(value, axis):
    slots = {0: value}
    bit = lax.axis_size(axis) // 2
    while bit:
        slots.update({j ^ bit: flip(v, axis, bit) for j, v in slots.items()})
        bit //= 2
    return [slots[j] for j in range(len(slots))]


def gather_ring(block, axis):
    count = lax.axis_size(axis)
    cycle = list(range(0, count, 2)) + list(range(count - 1, 0, -2))
    place = [cycle.index(i) for i in range(count)]
    ahead = [(cycle[r], cycle[(r + 1) % count]) for r in range(count)]
    behind = [(b, a) for a, b in ahead]
    mine = jnp.asarray(place, jnp.int32)[lax.axis_index(axis)]
    owner = jnp.asarray(cycle, jnp.int32)
    rows = block.shape[0]
    full = jnp.zeros((count, *block.shape), block.dtype)
    full = lax.dynamic_update_index_in_dim(full, block, lax.axis_index(axis), 0)
    up = down = block
    for step in range(1, (count + 1) // 2):
        up = lax.ppermute(up, axis, ahead)
        down = lax.ppermute(down, axis, behind)
        full = lax.dynamic_update_index_in_dim(full, up, owner[(mine - step) % count], 0)
        full = lax.dynamic_update_index_in_dim(full, down, owner[(mine + step) % count], 0)
    if count % 2 == 0:
        half = rows // 2
        up = lax.ppermute(up[:half], axis, ahead)
        down = lax.ppermute(down[half:], axis, behind)
        last = jnp.concatenate([up, down], axis=0)
        full = lax.dynamic_update_index_in_dim(full, last, owner[(mine + count // 2) % count], 0)
    return full.reshape(count * rows, *block.shape[1:])


def conv_section(frames, past, length, conv_weight):
    f_dev, height, width, channels = frames.shape
    joined = jnp.concatenate([past, frames], axis=0)
    act = jax.nn.silu(joined.astype(jnp.float32)).astype(jnp.bfloat16)
    padded = jnp.pad(act, ((0, 0), (1, 1), (1, 1), (0, 0)))
    frame_ids = lax.axis_index("ctx") * f_dev + jnp.arange(f_dev, dtype=jnp.int32)
    cells = f_dev * height * width
    total = jnp.zeros((cells, channels), jnp.float32)
    for lag in range(3):
        part = jnp.zeros((cells, channels), jnp.float32)
        for row in range(3):
            for col in range(3):
                slab = padded[
                    2 - lag : 2 - lag + f_dev, row : row + height, col : col + width, :
                ].reshape(-1, channels)
                part = part + jnp.dot(
                    slab, conv_weight[lag, row, col], preferred_element_type=jnp.float32
                )
        if lag == 0:
            total = part
        else:
            valid = ((frame_ids < length) & (frame_ids >= lag)).astype(jnp.float32)
            total = total + part * jnp.repeat(valid, height * width)[:, None]
    return (frames.astype(jnp.float32) + total.reshape(frames.shape)).astype(jnp.bfloat16)


def attend(qkv, lengths, frame_ids):
    query, keys, values = (qkv[..., i * HD : (i + 1) * HD] for i in range(3))
    scores = jnp.einsum(
        "gtphd,gsphd->gphts", query, keys, preferred_element_type=jnp.float32
    ) * HD ** (-0.5)
    video = frame_ids[None, :] < lengths[:, None]
    allowed = (
        video[:, :, None] & video[:, None, :] | (frame_ids[:, None] == frame_ids[None, :])[None]
    )
    scores = jnp.where(allowed[:, None, None], scores, -1e30)
    top = jnp.max(scores, axis=-1, keepdims=True)
    expo = jnp.exp(scores - top)
    probs = (expo / jnp.sum(expo, axis=-1, keepdims=True)).astype(jnp.bfloat16)
    return jnp.einsum(
        "gphts,gsphd->gtphd", probs, values, preferred_element_type=jnp.float32
    ).astype(jnp.bfloat16)


def to_owners(value, n, me):
    f_dev, tokens, features = value.shape
    blocks = value.reshape(f_dev, n, tokens // n, features)
    return [
        rotate(lax.dynamic_index_in_dim(blocks, (me + k) % n, 1, keepdims=False), "ctx", k)
        for k in range(n)
    ]


def on_device(
    frames, stream, video_frames, conv_weight, latent_weight, embed_weight, norm_gain, qkv_weight
):
    f_dev, height, width, channels = frames.shape[1:]
    tokens, width_model = stream.shape[2:]
    n, me = lax.axis_size("ctx"), lax.axis_index("ctx")
    groups, me_dp = lax.axis_size("dp"), lax.axis_index("dp")
    pos = tokens // n

    past = lax.ppermute(
        frames[0, f_dev - 2 :], "ctx", [(i, i + 1) for i in range(n - 1)]
    )
    pieces = to_owners(stream[0], n, me)
    pair = 2 if n % 2 == 0 else 1
    chunks = [jnp.stack(pieces[k : k + pair]) for k in range(0, n, pair)]
    spread = [butterfly(chunk, "dp") for chunk in chunks]
    streams = jnp.stack(
        [jnp.concatenate([chunk[j] for chunk in spread], axis=0) for j in range(groups)]
    ).reshape(-1, width_model)
    lengths = jnp.concatenate(butterfly(video_frames, "dp"))
    weight = gather_ring(qkv_weight, "ctx")

    section = conv_section(frames[0], past, video_frames[0], conv_weight)
    latent = jnp.dot(
        section.reshape(-1, channels), latent_weight, preferred_element_type=jnp.float32
    ).astype(jnp.bfloat16)
    lat = latent.shape[1]
    patches = (
        latent.reshape(f_dev, height // 2, 2, width // 2, 2, lat)
        .transpose(0, 1, 3, 2, 4, 5)
        .reshape(f_dev, tokens, 4 * lat)
    )
    patches = jnp.stack(butterfly(jnp.stack(to_owners(patches, n, me)), "dp")).reshape(-1, 4 * lat)

    embedded = jnp.dot(
        patches, embed_weight, preferred_element_type=jnp.float32
    ) + streams.astype(jnp.float32)
    scale = lax.rsqrt(jnp.mean(embedded * embedded, axis=-1, keepdims=True) + 1e-06)
    normed = (embedded * scale * norm_gain).astype(jnp.bfloat16)
    qkv = jnp.dot(normed, weight, preferred_element_type=jnp.float32).astype(jnp.bfloat16)
    heads = qkv_weight.shape[1] // (3 * HD)
    qkv = qkv.reshape(groups, n * f_dev, pos, heads, 3 * HD)

    slot_owner = (me - jnp.arange(n, dtype=jnp.int32)) % n
    frame_ids = (
        slot_owner[:, None] * f_dev + jnp.arange(f_dev, dtype=jnp.int32)[None, :]
    ).reshape(-1)
    out = attend(qkv, lengths, frame_ids).reshape(groups, n, f_dev, pos, heads * HD)

    back = jnp.stack([rotate(out[:, k], "ctx", -k) for k in range(n)])
    back = back[(jnp.arange(n, dtype=jnp.int32) - me) % n]
    back = back.transpose(1, 2, 0, 3, 4).reshape(groups, f_dev, tokens, heads * HD)
    mixed = jnp.stack([back[0]] + [flip(back[j], "dp", j) for j in range(1, groups)])
    mixed = mixed[jnp.arange(groups, dtype=jnp.int32) ^ me_dp]
    mixed = mixed.transpose(1, 2, 0, 3).reshape(1, f_dev, tokens, groups * heads * HD)
    return section[None], mixed


def solution(mesh):
    return jax.shard_map(
        on_device,
        mesh=mesh,
        in_specs=(
            P("dp", "ctx", None, None, None),
            P("dp", "ctx", None, None),
            P("dp"),
            P(),
            P(),
            P(),
            P(),
            P("ctx", "dp"),
        ),
        out_specs=(P("dp", "ctx", None, None, None), P("dp", "ctx", None, None)),
        check_vma=False,
    )
```

```python
import functools

import jax
import jax.numpy as jnp
from jax import lax
from jax.experimental import pallas as pl
from jax.experimental.pallas import tpu as pltpu
from jax.sharding import PartitionSpec as P

HD = 128
VMEM = pl.BlockSpec(memory_space=pltpu.VMEM)
HBM = pl.BlockSpec(memory_space=pltpu.HBM)
SMEM = pl.BlockSpec(memory_space=pltpu.SMEM)


def flip(value, axis, bit):
    count = lax.axis_size(axis)
    return lax.ppermute(value, axis, [(i, i ^ bit) for i in range(count)])


def ring_size(axis):
    count = lax.axis_size(axis)
    return count if count <= 8 and count % 2 == 0 else 0


def gather_ring(block, axis):
    count = ring_size(axis)
    if not count:
        return [lax.all_gather(block, axis, axis=0, tiled=True)]
    cycle = list(range(0, count, 2)) + list(range(count - 1, 0, -2))
    ahead = [(cycle[r], cycle[(r + 1) % count]) for r in range(count)]
    behind = [(b, a) for a, b in ahead]
    pieces = [block]
    up = down = block
    for _ in range(1, count // 2):
        up = lax.ppermute(up, axis, ahead)
        down = lax.ppermute(down, axis, behind)
        pieces += [up, down]
    half = block.shape[0] // 2
    pieces.append(lax.ppermute(up[:half], axis, ahead))
    pieces.append(lax.ppermute(down[half:], axis, behind))
    return pieces


def piece_rows(count, rows):
    if not count:
        return [0]
    me = lax.axis_index("ctx")
    place = jnp.where(lax.rem(me, 2) == 0, me // 2, count - 1 - me // 2)

    def owner(shift):
        spot = lax.rem(place + shift + count, count)
        return jnp.where(spot < count // 2, 2 * spot, 2 * (count - 1 - spot) + 1) * rows

    first = [me * rows]
    for step in range(1, count // 2):
        first += [owner(-step), owner(step)]
    far = owner(count // 2)
    return first + [far, far + rows // 2]


def conv_kernel(
    length_ref, past_ref, frames_ref, weight_ref, latent_weight_ref, section_ref, latent_ref,
    shifted, weights, near, lagged, sems,
):
    f_dev, height, width, channels = frames_ref.shape
    lags, side = past_ref.shape[0] + 1, 3
    taps = weight_ref.shape[0]
    cells = height * width

    def load(tap):
        return pltpu.make_async_copy(weight_ref.at[tap], weights.at[tap], sems.at[tap])

    for tap in range(taps):
        load(tap).start()
    column = lax.rem(lax.broadcasted_iota(jnp.int32, (cells, channels), 0), width)
    edge = jnp.zeros((width, channels), jnp.bfloat16)

    def prepare(source, slot):
        act = jax.nn.silu(source.astype(jnp.float32)).reshape(cells, channels)
        left = jnp.where(column == 0, 0.0, pltpu.roll(act, 1, 0))
        right = jnp.where(column == width - 1, 0.0, pltpu.roll(act, cells - 1, 0))
        for col, value in enumerate((left, act, right)):
            shifted[col, slot, 0] = edge
            shifted[col, slot, height + 1] = edge
            shifted[col, slot, 1 : height + 1] = value.astype(jnp.bfloat16).reshape(
                height, width, channels
            )

    @pl.loop(0, lags - 1)
    def _(slot):
        prepare(past_ref[slot], slot)

    @pl.loop(0, f_dev)
    def _(slot):
        prepare(frames_ref[slot], slot + lags - 1)

    def add(tap, total):
        load(tap).wait()
        lag, row, col = tap // (side * side), lax.rem(tap // side, side), lax.rem(tap, side)
        slab = shifted[col, pl.ds(lags - 1 - lag, f_dev), pl.ds(row, height)]
        total[...] += jnp.dot(
            slab.reshape(f_dev * cells, channels), weights[tap], preferred_element_type=jnp.float32
        )

    near[...] = jnp.zeros_like(near)
    lagged[...] = jnp.zeros_like(lagged)

    @pl.loop(0, side * side)
    def _(tap):
        add(tap, near)

    @pl.loop(side * side, taps)
    def _(tap):
        add(tap, lagged)

    first = lax.axis_index("ctx") * f_dev

    @pl.loop(0, f_dev)
    def _(slot):
        video = jnp.where(first + slot < length_ref[0], 1.0, 0.0)
        rows = pl.ds(pl.multiple_of(slot * cells, cells), cells)
        value = (
            frames_ref[slot].astype(jnp.float32).reshape(cells, channels)
            + near[rows]
            + video * lagged[rows]
        ).astype(jnp.bfloat16)
        section_ref[slot] = value.reshape(height, width, channels)
        latent_ref[rows] = jnp.dot(
            value, latent_weight_ref[...], preferred_element_type=jnp.float32
        ).astype(jnp.bfloat16)


def conv_section(frames, past, length, conv_weight, latent_weight):
    f_dev, height, width, channels = frames.shape
    lags = conv_weight.shape[0]
    taps = conv_weight.shape[0] * conv_weight.shape[1] * conv_weight.shape[2]
    cells = f_dev * height * width
    return pl.pallas_call(
        conv_kernel,
        out_shape=(
            jax.ShapeDtypeStruct(frames.shape, jnp.bfloat16),
            jax.ShapeDtypeStruct((cells, latent_weight.shape[1]), jnp.bfloat16),
        ),
        in_specs=[SMEM, VMEM, VMEM, HBM, VMEM],
        out_specs=(VMEM, VMEM),
        scratch_shapes=[
            pltpu.VMEM((3, f_dev + lags - 1, height + 2, width, channels), jnp.bfloat16),
            pltpu.VMEM((taps, channels, channels), jnp.bfloat16),
            pltpu.VMEM((cells, channels), jnp.float32),
            pltpu.VMEM((cells, channels), jnp.float32),
            pltpu.SemaphoreType.DMA((taps,)),
        ],
        compiler_params=pltpu.CompilerParams(vmem_limit_bytes=40 << 20),
        cost_estimate=pl.CostEstimate(
            flops=2 * cells * taps * channels * channels,
            bytes_accessed=2 * conv_weight.size,
            transcendentals=0,
        ),
        name="conv",
    )(length, past, frames, conv_weight.reshape(taps, channels, channels), latent_weight)


def norm_kernel(bounds, groups, patch_size, patches_ref, embed_ref, gain_ref, *refs):
    parts, (out_ref, held, embedded, sems) = refs[: len(bounds) * groups], refs[len(bounds) * groups :]
    me = lax.axis_index("dp")
    width = embed_ref.shape[1]
    n, f_dev, pos = held.shape[1:4]
    copies = []
    for c, (a, b) in enumerate(bounds):
        for j in range(groups):
            spot = c * groups + j
            copies.append(
                pltpu.make_async_copy(
                    parts[spot], held.at[lax.bitwise_xor(me, j), :, pl.ds(a, b - a)], sems.at[spot]
                )
            )
    for copy in copies:
        copy.start()
    tile = 256

    @pl.loop(0, width // tile)
    def _(i):
        columns = pl.ds(pl.multiple_of(i * tile, tile), tile)
        embedded[:, columns] = jnp.dot(
            patches_ref[:, :patch_size], embed_ref[:, columns], preferred_element_type=jnp.float32
        )

    for copy in copies:
        copy.wait()

    @pl.loop(0, groups * n)
    def _(i):
        group, device = i // n, lax.rem(i, n)

        @pl.loop(0, f_dev)
        def _(slot):
            rows = pl.ds(pl.multiple_of((i * f_dev + slot) * pos, pos), pos)
            value = embedded[rows] + held[group, device, slot].astype(jnp.float32)
            scale = lax.rsqrt(jnp.mean(value * value, axis=-1, keepdims=True) + 1e-06)
            out_ref[group, device, slot] = (value * scale * gain_ref[...]).astype(jnp.bfloat16)


def norm_rows(patches, embed_weight, norm_gain, parts, bounds, groups, n, f_dev, pos):
    width = embed_weight.shape[1]
    rows = groups * n * f_dev * pos
    if pos % 8:
        order = jnp.arange(groups, dtype=jnp.int32) ^ lax.axis_index("dp")
        chunks = [
            jnp.stack(parts[c * groups : (c + 1) * groups])[order] for c in range(len(bounds))
        ]
        held = jnp.concatenate(chunks, axis=2).reshape(rows, width)
        value = jnp.dot(
            patches[:, : embed_weight.shape[0]], embed_weight, preferred_element_type=jnp.float32
        ) + held.astype(jnp.float32)
        scale = lax.rsqrt(jnp.mean(value * value, axis=-1, keepdims=True) + 1e-06)
        return (value * scale * norm_gain).astype(jnp.bfloat16)
    return pl.pallas_call(
        functools.partial(norm_kernel, bounds, groups, embed_weight.shape[0]),
        out_shape=jax.ShapeDtypeStruct((groups, n, f_dev, pos, width), jnp.bfloat16),
        in_specs=[VMEM] * 3 + [HBM] * len(parts),
        out_specs=VMEM,
        scratch_shapes=[
            pltpu.VMEM((groups, n, f_dev, pos, width), jnp.bfloat16),
            pltpu.VMEM((rows, width), jnp.float32),
            pltpu.SemaphoreType.DMA((len(parts),)),
        ],
        compiler_params=pltpu.CompilerParams(vmem_limit_bytes=44 << 20),
        cost_estimate=pl.CostEstimate(
            flops=2 * rows * width * 512, bytes_accessed=4 * rows * width, transcendentals=0
        ),
        name="norm",
    )(patches, embed_weight, norm_gain[None], *parts)


def qkv_kernel(count, normed_ref, *refs):
    *pieces, out_ref, weight, sems = refs
    firsts = piece_rows(count, pieces[0].shape[0])
    copies = [
        pltpu.make_async_copy(
            piece, weight.at[pl.ds(pl.multiple_of(first, 64), piece.shape[0])], sems.at[i]
        )
        for i, (piece, first) in enumerate(zip(pieces, firsts))
    ]
    for copy in copies:
        copy.start()
    for copy in copies:
        copy.wait()
    rows = normed_ref.shape[0]
    tile = rows // 4 if rows % 64 == 0 else rows

    @pl.loop(0, rows // tile)
    def _(i):
        span = pl.ds(pl.multiple_of(i * tile, 16), tile)
        out_ref[span] = jnp.dot(
            normed_ref[span], weight[...], preferred_element_type=jnp.float32
        ).astype(jnp.bfloat16)


def project(normed, pieces, count):
    depth, columns = normed.shape[1], pieces[0].shape[1]
    return pl.pallas_call(
        functools.partial(qkv_kernel, count),
        out_shape=jax.ShapeDtypeStruct((normed.shape[0], columns), jnp.bfloat16),
        in_specs=[VMEM] + [HBM] * len(pieces),
        out_specs=VMEM,
        scratch_shapes=[
            pltpu.VMEM((depth, columns), jnp.bfloat16),
            pltpu.SemaphoreType.DMA((len(pieces),)),
        ],
        compiler_params=pltpu.CompilerParams(vmem_limit_bytes=32 << 20),
        cost_estimate=pl.CostEstimate(
            flops=2 * normed.size * columns,
            bytes_accessed=2 * (normed.size + depth * columns),
            transcendentals=0,
        ),
        name="qkv",
    )(normed, *pieces)


def attend(qkv, lengths):
    query, keys, values = (qkv[..., i * HD : (i + 1) * HD] for i in range(3))
    scores = jnp.einsum(
        "gtphd,gsphd->gphts", query, keys, preferred_element_type=jnp.float32
    ) * HD ** (-0.5)
    frame_ids = jnp.arange(qkv.shape[1], dtype=jnp.int32)
    video = frame_ids[None, :] < lengths[:, None]
    allowed = (
        video[:, :, None] & video[:, None, :] | (frame_ids[:, None] == frame_ids[None, :])[None]
    )
    scores = jnp.where(allowed[:, None, None], scores, -1e30)
    top = jnp.max(scores, axis=-1, keepdims=True)
    expo = jnp.exp(scores - top)
    probs = (expo / jnp.sum(expo, axis=-1, keepdims=True)).astype(jnp.bfloat16)
    return jnp.einsum(
        "gphts,gsphd->gtphd", probs, values, preferred_element_type=jnp.float32
    ).astype(jnp.bfloat16)


def body(
    frames, stream, video_frames, conv_weight, latent_weight, embed_weight, norm_gain, qkv_weight
):
    f_dev, height, width, _ = frames.shape[1:]
    tokens, width_model = stream.shape[2:]
    n, groups = lax.axis_size("ctx"), lax.axis_size("dp")
    pos = tokens // n
    heads = qkv_weight.shape[1] // (3 * HD)

    past = lax.ppermute(frames[0, f_dev - 2 :], "ctx", [(i, i + 1) for i in range(n - 1)])

    bounds = ((0, (f_dev + 1) // 2), ((f_dev + 1) // 2, f_dev))
    parts = []
    for first, end in bounds:
        blocks = stream[0, first:end].reshape(end - first, n, pos, width_model).transpose(1, 0, 2, 3)
        slots = {0: lax.all_to_all(blocks, "ctx", 0, 0)}
        bit = groups // 2
        while bit:
            for j in sorted(slots):
                slots[j ^ bit] = flip(slots[j], "dp", bit)
            bit //= 2
        parts += [slots[j] for j in range(groups)]

    pieces = gather_ring(qkv_weight, "ctx")

    section, latent = conv_section(frames[0], past, video_frames, conv_weight, latent_weight)
    lat = latent.shape[1]
    patches = (
        latent.reshape(f_dev, height // 2, 2, width // 2, 2, lat)
        .transpose(0, 1, 3, 2, 4, 5)
        .reshape(f_dev, n, pos, 4 * lat)
        .transpose(1, 0, 2, 3)
    )
    length = jnp.broadcast_to(video_frames.astype(jnp.bfloat16), (*patches.shape[:-1], 1))
    patches = jnp.concatenate([patches, length], axis=-1)
    patches = jnp.broadcast_to(patches[None], (groups, *patches.shape)).reshape(
        groups * n, f_dev, pos, -1
    )
    patches = lax.all_to_all(patches, ("dp", "ctx"), 0, 0, tiled=True)
    rows = groups * n * f_dev * pos
    patches = patches.reshape(rows, -1)
    lengths = patches[:: rows // groups, -1].astype(jnp.int32)

    normed = norm_rows(
        patches, embed_weight, norm_gain, parts, bounds, groups, n, f_dev, pos
    ).reshape(rows, width_model)
    qkv = project(normed, pieces, ring_size("ctx"))
    out = attend(qkv.reshape(groups, n * f_dev, pos, heads, 3 * HD), lengths)
    out = lax.all_to_all(
        out.reshape(groups * n, f_dev, pos, heads * HD), ("dp", "ctx"), 0, 0, tiled=True
    )
    out = out.reshape(groups, n, f_dev, pos, heads * HD).transpose(2, 1, 3, 0, 4)
    return section[None], out.reshape(1, f_dev, tokens, groups * heads * HD)


def solution(mesh):
    return jax.shard_map(
        body,
        mesh=mesh,
        in_specs=(
            P("dp", "ctx", None, None, None),
            P("dp", "ctx", None, None),
            P("dp"),
            P(),
            P(),
            P(),
            P(),
            P("ctx", "dp"),
        ),
        out_specs=(P("dp", "ctx", None, None, None), P("dp", "ctx", None, None)),
        check_vma=False,
    )
```

```python
import functools

import jax
import jax.numpy as jnp
from jax import lax
from jax.experimental import pallas as pl
from jax.experimental.pallas import tpu as pltpu
from jax.sharding import PartitionSpec as P

HD = 128
VMEM = pl.BlockSpec(memory_space=pltpu.VMEM)
HBM = pl.BlockSpec(memory_space=pltpu.HBM)
SMEM = pl.BlockSpec(memory_space=pltpu.SMEM)


def flip(value, axis, bit):
    count = lax.axis_size(axis)
    return lax.ppermute(value, axis, [(i, i ^ bit) for i in range(count)])


def ring_size(axis):
    count = lax.axis_size(axis)
    return count if count <= 8 and count % 2 == 0 else 0


def gather_ring(block, axis):
    count = ring_size(axis)
    if not count:
        return [lax.all_gather(block, axis, axis=0, tiled=True)]
    cycle = list(range(0, count, 2)) + list(range(count - 1, 0, -2))
    ahead = [(cycle[r], cycle[(r + 1) % count]) for r in range(count)]
    behind = [(b, a) for a, b in ahead]
    pieces = [block]
    up = down = block
    for _ in range(1, count // 2):
        up = lax.ppermute(up, axis, ahead)
        down = lax.ppermute(down, axis, behind)
        pieces += [up, down]
    half = block.shape[0] // 2
    pieces.append(lax.ppermute(up[:half], axis, ahead))
    pieces.append(lax.ppermute(down[half:], axis, behind))
    return pieces


def piece_rows(count, rows):
    if not count:
        return [0]
    me = lax.axis_index("ctx")
    place = jnp.where(lax.rem(me, 2) == 0, me // 2, count - 1 - me // 2)

    def owner(shift):
        spot = lax.rem(place + shift + count, count)
        return jnp.where(spot < count // 2, 2 * spot, 2 * (count - 1 - spot) + 1) * rows

    first = [me * rows]
    for step in range(1, count // 2):
        first += [owner(-step), owner(step)]
    far = owner(count // 2)
    return first + [far, far + rows // 2]


def conv_kernel(
    length_ref, past_ref, frames_ref, weight_ref, latent_weight_ref, section_ref, latent_ref,
    shifted, weights, near, lagged, sems,
):
    f_dev, height, width, channels = frames_ref.shape
    lags, side = past_ref.shape[0] + 1, 3
    taps = weight_ref.shape[0]
    cells = height * width

    def load(tap):
        return pltpu.make_async_copy(weight_ref.at[tap], weights.at[tap], sems.at[tap])

    for tap in range(taps):
        load(tap).start()
    column = lax.rem(lax.broadcasted_iota(jnp.int32, (cells, channels), 0), width)
    edge = jnp.zeros((width, channels), jnp.bfloat16)

    def prepare(source, slot):
        act = jax.nn.silu(source.astype(jnp.float32)).reshape(cells, channels)
        left = jnp.where(column == 0, 0.0, pltpu.roll(act, 1, 0))
        right = jnp.where(column == width - 1, 0.0, pltpu.roll(act, cells - 1, 0))
        for col, value in enumerate((left, act, right)):
            shifted[col, slot, 0] = edge
            shifted[col, slot, height + 1] = edge
            shifted[col, slot, 1 : height + 1] = value.astype(jnp.bfloat16).reshape(
                height, width, channels
            )

    @pl.loop(0, lags - 1)
    def _(slot):
        prepare(past_ref[slot], slot)

    @pl.loop(0, f_dev)
    def _(slot):
        prepare(frames_ref[slot], slot + lags - 1)

    def add(tap, total):
        load(tap).wait()
        lag, row, col = tap // (side * side), lax.rem(tap // side, side), lax.rem(tap, side)
        slab = shifted[col, pl.ds(lags - 1 - lag, f_dev), pl.ds(row, height)]
        total[...] += jnp.dot(
            slab.reshape(f_dev * cells, channels), weights[tap], preferred_element_type=jnp.float32
        )

    near[...] = jnp.zeros_like(near)
    lagged[...] = jnp.zeros_like(lagged)

    @pl.loop(0, side * side)
    def _(tap):
        add(tap, near)

    @pl.loop(side * side, taps)
    def _(tap):
        add(tap, lagged)

    first = lax.axis_index("ctx") * f_dev

    @pl.loop(0, f_dev)
    def _(slot):
        video = jnp.where(first + slot < length_ref[0], 1.0, 0.0)
        rows = pl.ds(pl.multiple_of(slot * cells, cells), cells)
        value = (
            frames_ref[slot].astype(jnp.float32).reshape(cells, channels)
            + near[rows]
            + video * lagged[rows]
        ).astype(jnp.bfloat16)
        section_ref[slot] = value.reshape(height, width, channels)
        latent_ref[rows] = jnp.dot(
            value, latent_weight_ref[...], preferred_element_type=jnp.float32
        ).astype(jnp.bfloat16)


def conv_section(frames, past, length, conv_weight, latent_weight):
    f_dev, height, width, channels = frames.shape
    lags = conv_weight.shape[0]
    taps = conv_weight.shape[0] * conv_weight.shape[1] * conv_weight.shape[2]
    cells = f_dev * height * width
    return pl.pallas_call(
        conv_kernel,
        out_shape=(
            jax.ShapeDtypeStruct(frames.shape, jnp.bfloat16),
            jax.ShapeDtypeStruct((cells, latent_weight.shape[1]), jnp.bfloat16),
        ),
        in_specs=[SMEM, VMEM, VMEM, HBM, VMEM],
        out_specs=(VMEM, VMEM),
        scratch_shapes=[
            pltpu.VMEM((3, f_dev + lags - 1, height + 2, width, channels), jnp.bfloat16),
            pltpu.VMEM((taps, channels, channels), jnp.bfloat16),
            pltpu.VMEM((cells, channels), jnp.float32),
            pltpu.VMEM((cells, channels), jnp.float32),
            pltpu.SemaphoreType.DMA((taps,)),
        ],
        compiler_params=pltpu.CompilerParams(vmem_limit_bytes=40 << 20),
        cost_estimate=pl.CostEstimate(
            flops=2 * cells * taps * channels * channels,
            bytes_accessed=2 * conv_weight.size,
            transcendentals=0,
        ),
        name="conv",
    )(length, past, frames, conv_weight.reshape(taps, channels, channels), latent_weight)


def norm_kernel(groups, patch_size, patches_ref, embed_ref, gain_ref, *refs):
    parts, (out_ref, held, embedded, sems) = refs[:groups], refs[groups:]
    me = lax.axis_index("dp")
    width = embed_ref.shape[1]
    n, f_dev, pos = held.shape[1:4]
    copies = [
        pltpu.make_async_copy(parts[j], held.at[lax.bitwise_xor(me, j)], sems.at[j])
        for j in range(groups)
    ]
    for copy in copies:
        copy.start()
    tile = 256

    @pl.loop(0, width // tile)
    def _(i):
        columns = pl.ds(pl.multiple_of(i * tile, tile), tile)
        embedded[:, columns] = jnp.dot(
            patches_ref[:, :patch_size], embed_ref[:, columns], preferred_element_type=jnp.float32
        )

    for copy in copies:
        copy.wait()
    block = f_dev * pos

    @pl.loop(0, groups * n)
    def _(i):
        group, device = i // n, lax.rem(i, n)
        rows = pl.ds(pl.multiple_of(i * block, pos), block)
        stream = held[group, device].astype(jnp.float32).reshape(block, width)
        value = embedded[rows] + stream
        scale = lax.rsqrt(jnp.mean(value * value, axis=-1, keepdims=True) + 1e-06)
        value = value * scale * gain_ref[...]
        out_ref[group, device] = value.reshape(f_dev, pos, width).astype(jnp.bfloat16)


def norm_rows(patches, embed_weight, norm_gain, parts):
    groups, (n, f_dev, pos, width) = len(parts), parts[0].shape
    rows = groups * n * f_dev * pos
    if pos % 8:
        order = jnp.arange(groups, dtype=jnp.int32) ^ lax.axis_index("dp")
        held = jnp.stack(parts)[order].reshape(rows, width)
        value = jnp.dot(
            patches[:, : embed_weight.shape[0]], embed_weight, preferred_element_type=jnp.float32
        ) + held.astype(jnp.float32)
        scale = lax.rsqrt(jnp.mean(value * value, axis=-1, keepdims=True) + 1e-06)
        return (value * scale * norm_gain).astype(jnp.bfloat16)
    return pl.pallas_call(
        functools.partial(norm_kernel, groups, embed_weight.shape[0]),
        out_shape=jax.ShapeDtypeStruct((groups, n, f_dev, pos, width), jnp.bfloat16),
        in_specs=[VMEM] * 3 + [HBM] * groups,
        out_specs=VMEM,
        scratch_shapes=[
            pltpu.VMEM((groups, n, f_dev, pos, width), jnp.bfloat16),
            pltpu.VMEM((rows, width), jnp.float32),
            pltpu.SemaphoreType.DMA((groups,)),
        ],
        compiler_params=pltpu.CompilerParams(vmem_limit_bytes=44 << 20),
        cost_estimate=pl.CostEstimate(
            flops=2 * rows * width * 512, bytes_accessed=4 * rows * width, transcendentals=0
        ),
        name="norm",
    )(patches, embed_weight, norm_gain[None], *parts).reshape(rows, width)


def qkv_kernel(count, spots, has_total, normed_ref, *refs):
    refs = list(refs)
    total_ref = refs.pop(0) if has_total else None
    sems, weight, out_ref = refs.pop(), refs.pop(), refs.pop()
    depth = weight.shape[1]
    firsts = piece_rows(count, depth)
    copies, used = [], 0
    for i, pieces in enumerate(spots):
        row = 0
        for _ in pieces:
            piece = refs[used]
            copies.append(
                pltpu.make_async_copy(
                    piece, weight.at[i, pl.ds(row, piece.shape[0])], sems.at[used]
                )
            )
            row += piece.shape[0]
            used += 1
    for copy in copies:
        copy.start()
    for copy in copies:
        copy.wait()
    rows = normed_ref.shape[0]
    tile = rows // 4 if rows % 64 == 0 else rows

    @pl.loop(0, rows // tile)
    def _(i):
        span = pl.ds(pl.multiple_of(i * tile, 16), tile)
        total = total_ref[span] if has_total else None
        for j, pieces in enumerate(spots):
            first = firsts[pieces[0]]
            if count:
                first = pl.multiple_of(first, 128)
            product = jnp.dot(
                normed_ref[span, pl.ds(first, depth)], weight[j], preferred_element_type=jnp.float32
            )
            total = product if total is None else total + product
        out_ref[span] = total.astype(out_ref.dtype)


def project(normed, pieces, count, spots, total, is_last):
    depth, columns = pieces[0].shape
    chosen = [pieces[i] for spot in spots for i in spot]
    first = [] if total is None else [total]
    dtype = jnp.bfloat16 if is_last else jnp.float32
    return pl.pallas_call(
        functools.partial(qkv_kernel, count, spots, total is not None),
        out_shape=jax.ShapeDtypeStruct((normed.shape[0], columns), dtype),
        in_specs=[VMEM] * (1 + len(first)) + [HBM] * len(chosen),
        out_specs=VMEM,
        scratch_shapes=[
            pltpu.VMEM((len(spots), depth, columns), jnp.bfloat16),
            pltpu.SemaphoreType.DMA((len(chosen),)),
        ],
        compiler_params=pltpu.CompilerParams(vmem_limit_bytes=32 << 20),
        cost_estimate=pl.CostEstimate(
            flops=2 * normed.shape[0] * len(spots) * depth * columns,
            bytes_accessed=2 * normed.size,
            transcendentals=0,
        ),
        name="qkv",
    )(normed, *first, *chosen)


def project_all(normed, pieces, count):
    if not count:
        return project(normed, pieces, count, ((0,),), None, True)
    last = len(pieces) - 2
    early = max(1, last - 2)
    stages = [tuple((i,) for i in range(early))]
    if early < last:
        stages.append(tuple((i,) for i in range(early, last)))
    stages.append(((last, last + 1),))
    total = None
    for s, spots in enumerate(stages):
        total = project(normed, pieces, count, spots, total, s == len(stages) - 1)
    return total


def attend(qkv, lengths):
    query, keys, values = (qkv[..., i * HD : (i + 1) * HD] for i in range(3))
    scores = jnp.einsum(
        "gtphd,gsphd->gphts", query, keys, preferred_element_type=jnp.float32
    ) * HD ** (-0.5)
    frame_ids = jnp.arange(qkv.shape[1], dtype=jnp.int32)
    video = frame_ids[None, :] < lengths[:, None]
    allowed = (
        video[:, :, None] & video[:, None, :] | (frame_ids[:, None] == frame_ids[None, :])[None]
    )
    scores = jnp.where(allowed[:, None, None], scores, -1e30)
    top = jnp.max(scores, axis=-1, keepdims=True)
    expo = jnp.exp(scores - top)
    probs = (expo / jnp.sum(expo, axis=-1, keepdims=True)).astype(jnp.bfloat16)
    return jnp.einsum(
        "gphts,gsphd->gtphd", probs, values, preferred_element_type=jnp.float32
    ).astype(jnp.bfloat16)


def body(
    frames, stream, video_frames, conv_weight, latent_weight, embed_weight, norm_gain, qkv_weight
):
    f_dev, height, width, _ = frames.shape[1:]
    tokens, width_model = stream.shape[2:]
    n, groups = lax.axis_size("ctx"), lax.axis_size("dp")
    pos = tokens // n
    heads = qkv_weight.shape[1] // (3 * HD)

    past = lax.ppermute(frames[0, f_dev - 2 :], "ctx", [(i, i + 1) for i in range(n - 1)])

    blocks = stream[0].reshape(f_dev, n, pos, width_model).transpose(1, 0, 2, 3)
    slots = {0: lax.all_to_all(blocks, "ctx", 0, 0)}
    bit = groups // 2
    while bit:
        for j in sorted(slots):
            slots[j ^ bit] = flip(slots[j], "dp", bit)
        bit //= 2
    parts = [slots[j] for j in range(groups)]

    pieces = gather_ring(qkv_weight, "ctx")

    section, latent = conv_section(frames[0], past, video_frames, conv_weight, latent_weight)
    lat = latent.shape[1]
    patches = (
        latent.reshape(f_dev, height // 2, 2, width // 2, 2, lat)
        .transpose(0, 1, 3, 2, 4, 5)
        .reshape(f_dev, n, pos, 4 * lat)
        .transpose(1, 0, 2, 3)
    )
    length = jnp.broadcast_to(video_frames.astype(jnp.bfloat16), (*patches.shape[:-1], 1))
    patches = jnp.concatenate([patches, length], axis=-1)
    patches = jnp.broadcast_to(patches[None], (groups, *patches.shape)).reshape(
        groups * n, f_dev, pos, -1
    )
    patches = lax.all_to_all(patches, ("dp", "ctx"), 0, 0, tiled=True)
    rows = groups * n * f_dev * pos
    patches = patches.reshape(rows, -1)
    lengths = patches[:: rows // groups, -1].astype(jnp.int32)

    normed = norm_rows(patches, embed_weight, norm_gain, parts)
    qkv = project_all(normed, pieces, ring_size("ctx"))
    out = attend(qkv.reshape(groups, n * f_dev, pos, heads, 3 * HD), lengths)
    out = lax.all_to_all(
        out.reshape(groups * n, f_dev, pos, heads * HD), ("dp", "ctx"), 0, 0, tiled=True
    )
    out = out.reshape(groups, n, f_dev, pos, heads * HD).transpose(2, 1, 3, 0, 4)
    return section[None], out.reshape(1, f_dev, tokens, groups * heads * HD)


def solution(mesh):
    return jax.shard_map(
        body,
        mesh=mesh,
        in_specs=(
            P("dp", "ctx", None, None, None),
            P("dp", "ctx", None, None),
            P("dp"),
            P(),
            P(),
            P(),
            P(),
            P("ctx", "dp"),
        ),
        out_specs=(P("dp", "ctx", None, None, None), P("dp", "ctx", None, None)),
        check_vma=False,
    )
```

```python
import functools

import jax
import jax.numpy as jnp
from jax import lax
from jax.experimental import pallas as pl
from jax.experimental.pallas import tpu as pltpu
from jax.sharding import PartitionSpec as P

HD = 128
VMEM = pl.BlockSpec(memory_space=pltpu.VMEM)
HBM = pl.BlockSpec(memory_space=pltpu.HBM)
SMEM = pl.BlockSpec(memory_space=pltpu.SMEM)


def flip(value, axis, bit):
    count = lax.axis_size(axis)
    return lax.ppermute(value, axis, [(i, i ^ bit) for i in range(count)])


def ring_size(axis):
    count = lax.axis_size(axis)
    return count if count <= 8 and count % 2 == 0 else 0


def gather_ring(block, axis):
    count = ring_size(axis)
    if not count:
        return [lax.all_gather(block, axis, axis=0, tiled=True)]
    cycle = list(range(0, count, 2)) + list(range(count - 1, 0, -2))
    ahead = [(cycle[r], cycle[(r + 1) % count]) for r in range(count)]
    behind = [(b, a) for a, b in ahead]
    pieces = [block]
    up = down = block
    for _ in range(1, count // 2):
        up = lax.ppermute(up, axis, ahead)
        down = lax.ppermute(down, axis, behind)
        pieces += [up, down]
    half = block.shape[0] // 2
    pieces.append(lax.ppermute(up[:half], axis, ahead))
    pieces.append(lax.ppermute(down[half:], axis, behind))
    return pieces


def piece_rows(count, rows):
    if not count:
        return [0]
    me = lax.axis_index("ctx")
    place = jnp.where(lax.rem(me, 2) == 0, me // 2, count - 1 - me // 2)

    def owner(shift):
        spot = lax.rem(place + shift + count, count)
        return jnp.where(spot < count // 2, 2 * spot, 2 * (count - 1 - spot) + 1) * rows

    first = [me * rows]
    for step in range(1, count // 2):
        first += [owner(-step), owner(step)]
    far = owner(count // 2)
    return first + [far, far + rows // 2]


def load_taps(weight_ref, weights, sems, first):
    def load(tap):
        return pltpu.make_async_copy(weight_ref.at[first + tap], weights.at[tap], sems.at[tap])

    for tap in range(weights.shape[0]):
        load(tap).start()
    return load


def shift_into(shifted, source, slot):
    height, width, channels = source.shape
    cells = height * width
    column = lax.rem(lax.broadcasted_iota(jnp.int32, (cells, channels), 0), width)
    edge = jnp.zeros((width, channels), jnp.bfloat16)
    act = jax.nn.silu(source.astype(jnp.float32)).reshape(cells, channels)
    left = jnp.where(column == 0, 0.0, pltpu.roll(act, 1, 0))
    right = jnp.where(column == width - 1, 0.0, pltpu.roll(act, cells - 1, 0))
    for col, value in enumerate((left, act, right)):
        shifted[col, slot, 0] = edge
        shifted[col, slot, height + 1] = edge
        shifted[col, slot, 1 : height + 1] = value.astype(jnp.bfloat16).reshape(source.shape)


def add_tap(total, shifted, weights, load, tap, start, row, col, f_dev, height):
    load(tap).wait()
    slab = shifted[col, pl.ds(start, f_dev), pl.ds(row, height)]
    total[...] += jnp.dot(
        slab.reshape(total.shape[0], slab.shape[-1]),
        weights[tap],
        preferred_element_type=jnp.float32,
    )


def near_kernel(frames_ref, weight_ref, near_ref, shifted, weights, sems):
    f_dev, height = frames_ref.shape[:2]
    load = load_taps(weight_ref, weights, sems, 0)

    @pl.loop(0, f_dev)
    def _(slot):
        shift_into(shifted, frames_ref[slot], slot)

    near_ref[...] = jnp.zeros_like(near_ref)

    @pl.loop(0, weights.shape[0])
    def _(tap):
        add_tap(near_ref, shifted, weights, load, tap, 0, tap // 3, lax.rem(tap, 3), f_dev, height)


def lagged_kernel(
    length_ref, past_ref, frames_ref, weight_ref, latent_weight_ref, near_ref, section_ref,
    latent_ref, shifted, weights, total, sems,
):
    f_dev, height, width, channels = frames_ref.shape
    lags, cells = past_ref.shape[0], height * width
    load = load_taps(weight_ref, weights, sems, 9)

    @pl.loop(0, lags)
    def _(slot):
        shift_into(shifted, past_ref[slot], slot)

    @pl.loop(0, f_dev - 1)
    def _(slot):
        shift_into(shifted, frames_ref[slot], slot + lags)

    total[...] = jnp.zeros_like(total)

    @pl.loop(0, weights.shape[0])
    def _(tap):
        start = lags - 1 - tap // 9
        add_tap(
            total, shifted, weights, load, tap, start, lax.rem(tap // 3, 3), lax.rem(tap, 3),
            f_dev, height,
        )

    first = lax.axis_index("ctx") * f_dev

    @pl.loop(0, f_dev)
    def _(slot):
        video = jnp.where(first + slot < length_ref[0], 1.0, 0.0)
        rows = pl.ds(pl.multiple_of(slot * cells, cells), cells)
        value = (
            frames_ref[slot].astype(jnp.float32).reshape(cells, channels)
            + near_ref[rows]
            + video * total[rows]
        ).astype(jnp.bfloat16)
        section_ref[slot] = value.reshape(height, width, channels)
        latent_ref[rows] = jnp.dot(
            value, latent_weight_ref[...], preferred_element_type=jnp.float32
        ).astype(jnp.bfloat16)


def conv_section(frames, past, length, conv_weight, latent_weight):
    f_dev, height, width, channels = frames.shape
    lags = past.shape[0]
    cells = f_dev * height * width
    weight = conv_weight.reshape(-1, channels, channels)

    def scratch(slots, taps):
        return [
            pltpu.VMEM((3, slots, height + 2, width, channels), jnp.bfloat16),
            pltpu.VMEM((taps, channels, channels), jnp.bfloat16),
        ]

    def cost(taps):
        return pl.CostEstimate(
            flops=2 * cells * taps * channels * channels,
            bytes_accessed=2 * taps * channels * channels,
            transcendentals=0,
        )

    near = pl.pallas_call(
        near_kernel,
        out_shape=jax.ShapeDtypeStruct((cells, channels), jnp.float32),
        in_specs=[VMEM, HBM],
        out_specs=VMEM,
        scratch_shapes=[*scratch(f_dev, 9), pltpu.SemaphoreType.DMA((9,))],
        compiler_params=pltpu.CompilerParams(vmem_limit_bytes=24 << 20),
        cost_estimate=cost(9),
        name="near",
    )(frames, weight)
    return pl.pallas_call(
        lagged_kernel,
        out_shape=(
            jax.ShapeDtypeStruct(frames.shape, jnp.bfloat16),
            jax.ShapeDtypeStruct((cells, latent_weight.shape[1]), jnp.bfloat16),
        ),
        in_specs=[SMEM, VMEM, VMEM, HBM, VMEM, VMEM],
        out_specs=(VMEM, VMEM),
        scratch_shapes=[
            *scratch(f_dev + lags - 1, 9 * lags),
            pltpu.VMEM((cells, channels), jnp.float32),
            pltpu.SemaphoreType.DMA((9 * lags,)),
        ],
        compiler_params=pltpu.CompilerParams(vmem_limit_bytes=36 << 20),
        cost_estimate=cost(9 * lags),
        name="lagged",
    )(length, past, frames, weight, latent_weight, near)


def deal_kernel(stream_ref, *outs):
    n = len(outs)
    me = lax.axis_index("ctx")
    for k, out in enumerate(outs):
        out[...] = stream_ref[:, lax.rem(me + k, n)]


def deal(blocks):
    f_dev, n, pos, width = blocks.shape
    shape = jax.ShapeDtypeStruct((f_dev, pos, width), blocks.dtype)
    return pl.pallas_call(
        deal_kernel,
        out_shape=(shape,) * n,
        in_specs=[VMEM],
        out_specs=(VMEM,) * n,
        compiler_params=pltpu.CompilerParams(vmem_limit_bytes=10 << 20),
        cost_estimate=pl.CostEstimate(
            flops=blocks.size, bytes_accessed=4 * blocks.size, transcendentals=0
        ),
        name="deal",
    )(blocks)


def to_owners(blocks):
    n = blocks.shape[1]
    if n > 8:
        return None, [lax.all_to_all(blocks.transpose(1, 0, 2, 3), "ctx", 0, 0)]
    pieces = deal(blocks)
    near_first = sorted(range(n), key=lambda k: (min(k, n - k), -k))
    halves = [near_first[: n // 2], near_first[n // 2 :]]
    moved = []
    for turns in halves:
        rows = [
            lax.ppermute(pieces[k], "ctx", [(i, (i + k) % n) for i in range(n)])
            if k
            else pieces[0]
            for k in turns
        ]
        moved.append(jnp.stack(rows))
    return halves, moved


def norm_kernel(halves, groups, patch_size, patches_ref, embed_ref, gain_ref, *refs):
    parts, (out_ref, held, embedded, sems) = refs[:-4], refs[-4:]
    me, me_ctx = lax.axis_index("dp"), lax.axis_index("ctx")
    width = embed_ref.shape[1]
    n, f_dev, pos = held.shape[1:4]
    copies = []
    for spot, part in enumerate(parts):
        group = lax.bitwise_xor(me, spot % groups)
        if halves is None:
            copies.append((part, held.at[group]))
            continue
        for i, k in enumerate(halves[spot // groups]):
            copies.append((part.at[i], held.at[group, lax.rem(me_ctx - k + n, n)]))
    copies = [pltpu.make_async_copy(a, b, sems.at[i]) for i, (a, b) in enumerate(copies)]
    for copy in copies:
        copy.start()
    tile = 256

    @pl.loop(0, width // tile)
    def _(i):
        columns = pl.ds(pl.multiple_of(i * tile, tile), tile)
        embedded[:, columns] = jnp.dot(
            patches_ref[:, :patch_size], embed_ref[:, columns], preferred_element_type=jnp.float32
        )

    for copy in copies:
        copy.wait()
    block = f_dev * pos

    @pl.loop(0, groups * n)
    def _(i):
        group, device = i // n, lax.rem(i, n)
        rows = pl.ds(pl.multiple_of(i * block, pos), block)
        stream = held[group, device].astype(jnp.float32).reshape(block, width)
        value = embedded[rows] + stream
        scale = lax.rsqrt(jnp.mean(value * value, axis=-1, keepdims=True) + 1e-06)
        value = value * scale * gain_ref[...]
        out_ref[group, device] = value.reshape(f_dev, pos, width).astype(jnp.bfloat16)


def norm_rows(patches, embed_weight, norm_gain, halves, parts, groups, n):
    f_dev, pos, width = parts[0].shape[1:]
    rows = groups * n * f_dev * pos
    if pos % 8:
        order = jnp.arange(groups, dtype=jnp.int32) ^ lax.axis_index("dp")
        held = jnp.stack(parts)[order].reshape(rows, width)
        value = jnp.dot(
            patches[:, : embed_weight.shape[0]], embed_weight, preferred_element_type=jnp.float32
        ) + held.astype(jnp.float32)
        scale = lax.rsqrt(jnp.mean(value * value, axis=-1, keepdims=True) + 1e-06)
        return (value * scale * norm_gain).astype(jnp.bfloat16)
    return pl.pallas_call(
        functools.partial(norm_kernel, halves, groups, embed_weight.shape[0]),
        out_shape=jax.ShapeDtypeStruct((groups, n, f_dev, pos, width), jnp.bfloat16),
        in_specs=[VMEM] * 3 + [HBM] * len(parts),
        out_specs=VMEM,
        scratch_shapes=[
            pltpu.VMEM((groups, n, f_dev, pos, width), jnp.bfloat16),
            pltpu.VMEM((rows, width), jnp.float32),
            pltpu.SemaphoreType.DMA((groups * n,)),
        ],
        compiler_params=pltpu.CompilerParams(vmem_limit_bytes=44 << 20),
        cost_estimate=pl.CostEstimate(
            flops=2 * rows * width * 512, bytes_accessed=4 * rows * width, transcendentals=0
        ),
        name="norm",
    )(patches, embed_weight, norm_gain[None], *parts).reshape(rows, width)


def qkv_kernel(count, spots, has_total, normed_ref, *refs):
    refs = list(refs)
    total_ref = refs.pop(0) if has_total else None
    sems, weight, out_ref = refs.pop(), refs.pop(), refs.pop()
    depth = weight.shape[1]
    firsts = piece_rows(count, depth)
    copies, used = [], 0
    for i, pieces in enumerate(spots):
        row = 0
        for _ in pieces:
            piece = refs[used]
            copies.append(
                pltpu.make_async_copy(
                    piece, weight.at[i, pl.ds(row, piece.shape[0])], sems.at[used]
                )
            )
            row += piece.shape[0]
            used += 1
    for copy in copies:
        copy.start()
    for copy in copies:
        copy.wait()
    rows = normed_ref.shape[0]
    tile = rows // 4 if rows % 64 == 0 else rows

    @pl.loop(0, rows // tile)
    def _(i):
        span = pl.ds(pl.multiple_of(i * tile, 16), tile)
        total = total_ref[span] if has_total else None
        for j, pieces in enumerate(spots):
            first = firsts[pieces[0]]
            if count:
                first = pl.multiple_of(first, 128)
            product = jnp.dot(
                normed_ref[span, pl.ds(first, depth)], weight[j], preferred_element_type=jnp.float32
            )
            total = product if total is None else total + product
        out_ref[span] = total.astype(out_ref.dtype)


def project(normed, pieces, count, spots, total, is_last):
    depth, columns = pieces[0].shape
    chosen = [pieces[i] for spot in spots for i in spot]
    first = [] if total is None else [total]
    dtype = jnp.bfloat16 if is_last else jnp.float32
    return pl.pallas_call(
        functools.partial(qkv_kernel, count, spots, total is not None),
        out_shape=jax.ShapeDtypeStruct((normed.shape[0], columns), dtype),
        in_specs=[VMEM] * (1 + len(first)) + [HBM] * len(chosen),
        out_specs=VMEM,
        scratch_shapes=[
            pltpu.VMEM((len(spots), depth, columns), jnp.bfloat16),
            pltpu.SemaphoreType.DMA((len(chosen),)),
        ],
        compiler_params=pltpu.CompilerParams(vmem_limit_bytes=32 << 20),
        cost_estimate=pl.CostEstimate(
            flops=2 * normed.shape[0] * len(spots) * depth * columns,
            bytes_accessed=2 * normed.size,
            transcendentals=0,
        ),
        name="qkv",
    )(normed, *first, *chosen)


def project_all(normed, pieces, count):
    if not count:
        return project(normed, pieces, count, ((0,),), None, True)
    last = len(pieces) - 2
    early = max(1, last - 2)
    stages = [tuple((i,) for i in range(early))]
    if early < last:
        stages.append(tuple((i,) for i in range(early, last)))
    stages.append(((last, last + 1),))
    total = None
    for s, spots in enumerate(stages):
        total = project(normed, pieces, count, spots, total, s == len(stages) - 1)
    return total


def attend(qkv, lengths):
    query, keys, values = (qkv[..., i * HD : (i + 1) * HD] for i in range(3))
    scores = jnp.einsum(
        "gtphd,gsphd->gphts", query, keys, preferred_element_type=jnp.float32
    ) * HD ** (-0.5)
    frame_ids = jnp.arange(qkv.shape[1], dtype=jnp.int32)
    video = frame_ids[None, :] < lengths[:, None]
    allowed = (
        video[:, :, None] & video[:, None, :] | (frame_ids[:, None] == frame_ids[None, :])[None]
    )
    scores = jnp.where(allowed[:, None, None], scores, -1e30)
    top = jnp.max(scores, axis=-1, keepdims=True)
    expo = jnp.exp(scores - top)
    probs = (expo / jnp.sum(expo, axis=-1, keepdims=True)).astype(jnp.bfloat16)
    return jnp.einsum(
        "gphts,gsphd->gtphd", probs, values, preferred_element_type=jnp.float32
    ).astype(jnp.bfloat16)


def body(
    frames, stream, video_frames, conv_weight, latent_weight, embed_weight, norm_gain, qkv_weight
):
    f_dev, height, width, _ = frames.shape[1:]
    tokens, width_model = stream.shape[2:]
    n, groups = lax.axis_size("ctx"), lax.axis_size("dp")
    pos = tokens // n
    heads = qkv_weight.shape[1] // (3 * HD)

    past = lax.ppermute(frames[0, f_dev - 2 :], "ctx", [(i, i + 1) for i in range(n - 1)])

    halves, moved = to_owners(stream[0].reshape(f_dev, n, pos, width_model))
    parts = []
    for value in moved:
        slots = {0: value}
        bit = groups // 2
        while bit:
            for j in sorted(slots):
                slots[j ^ bit] = flip(slots[j], "dp", bit)
            bit //= 2
        parts += [slots[j] for j in range(groups)]

    pieces = gather_ring(qkv_weight, "ctx")

    section, latent = conv_section(frames[0], past, video_frames, conv_weight, latent_weight)
    lat = latent.shape[1]
    patches = (
        latent.reshape(f_dev, height // 2, 2, width // 2, 2, lat)
        .transpose(0, 1, 3, 2, 4, 5)
        .reshape(f_dev, n, pos, 4 * lat)
        .transpose(1, 0, 2, 3)
    )
    length = jnp.broadcast_to(video_frames.astype(jnp.bfloat16), (*patches.shape[:-1], 1))
    patches = jnp.concatenate([patches, length], axis=-1)
    patches = jnp.broadcast_to(patches[None], (groups, *patches.shape)).reshape(
        groups * n, f_dev, pos, -1
    )
    patches = lax.all_to_all(patches, ("dp", "ctx"), 0, 0, tiled=True)
    rows = groups * n * f_dev * pos
    patches = patches.reshape(rows, -1)
    lengths = patches[:: rows // groups, -1].astype(jnp.int32)

    normed = norm_rows(patches, embed_weight, norm_gain, halves, parts, groups, n)
    qkv = project_all(normed, pieces, ring_size("ctx"))
    out = attend(qkv.reshape(groups, n * f_dev, pos, heads, 3 * HD), lengths)
    out = lax.all_to_all(
        out.reshape(groups * n, f_dev, pos, heads * HD), ("dp", "ctx"), 0, 0, tiled=True
    )
    out = out.reshape(groups, n, f_dev, pos, heads * HD).transpose(2, 1, 3, 0, 4)
    return section[None], out.reshape(1, f_dev, tokens, groups * heads * HD)


def solution(mesh):
    return jax.shard_map(
        body,
        mesh=mesh,
        in_specs=(
            P("dp", "ctx", None, None, None),
            P("dp", "ctx", None, None),
            P("dp"),
            P(),
            P(),
            P(),
            P(),
            P("ctx", "dp"),
        ),
        out_specs=(P("dp", "ctx", None, None, None), P("dp", "ctx", None, None)),
        check_vma=False,
    )
```

```python
import functools

import jax
import jax.numpy as jnp
from jax import lax
from jax.experimental import pallas as pl
from jax.experimental.pallas import tpu as pltpu
from jax.sharding import PartitionSpec as P

HD = 128
VMEM = pl.BlockSpec(memory_space=pltpu.VMEM)
HBM = pl.BlockSpec(memory_space=pltpu.HBM)
SMEM = pl.BlockSpec(memory_space=pltpu.SMEM)


def flip(value, axis, bit):
    count = lax.axis_size(axis)
    return lax.ppermute(value, axis, [(i, i ^ bit) for i in range(count)])


def ring_size(axis):
    count = lax.axis_size(axis)
    return count if count <= 8 and count % 2 == 0 else 0


def gather_ring(block, axis):
    count = ring_size(axis)
    if not count:
        return [lax.all_gather(block, axis, axis=0, tiled=True)]
    cycle = list(range(0, count, 2)) + list(range(count - 1, 0, -2))
    ahead = [(cycle[r], cycle[(r + 1) % count]) for r in range(count)]
    behind = [(b, a) for a, b in ahead]
    pieces = [block]
    up = down = block
    for _ in range(1, count // 2):
        up = lax.ppermute(up, axis, ahead)
        down = lax.ppermute(down, axis, behind)
        pieces += [up, down]
    half = block.shape[0] // 2
    pieces.append(lax.ppermute(up[:half], axis, ahead))
    pieces.append(lax.ppermute(down[half:], axis, behind))
    return pieces


def piece_rows(count, rows):
    if not count:
        return [0]
    me = lax.axis_index("ctx")
    place = jnp.where(lax.rem(me, 2) == 0, me // 2, count - 1 - me // 2)

    def owner(shift):
        spot = lax.rem(place + shift + count, count)
        return jnp.where(spot < count // 2, 2 * spot, 2 * (count - 1 - spot) + 1) * rows

    first = [me * rows]
    for step in range(1, count // 2):
        first += [owner(-step), owner(step)]
    far = owner(count // 2)
    return first + [far, far + rows // 2]


def load_taps(weight_ref, weights, sems, first):
    def load(tap):
        return pltpu.make_async_copy(weight_ref.at[first + tap], weights.at[tap], sems.at[tap])

    for tap in range(weights.shape[0]):
        load(tap).start()
    return load


def shift_into(shifted, source, slot):
    height, width, channels = source.shape
    cells = height * width
    column = lax.rem(lax.broadcasted_iota(jnp.int32, (cells, channels), 0), width)
    edge = jnp.zeros((width, channels), jnp.bfloat16)
    act = jax.nn.silu(source.astype(jnp.float32)).reshape(cells, channels)
    left = jnp.where(column == 0, 0.0, pltpu.roll(act, 1, 0))
    right = jnp.where(column == width - 1, 0.0, pltpu.roll(act, cells - 1, 0))
    for col, value in enumerate((left, act, right)):
        shifted[col, slot, 0] = edge
        shifted[col, slot, height + 1] = edge
        shifted[col, slot, 1 : height + 1] = value.astype(jnp.bfloat16).reshape(source.shape)


def add_tap(total, shifted, weights, load, tap, start, row, col, f_dev, height):
    load(tap).wait()
    slab = shifted[col, pl.ds(start, f_dev), pl.ds(row, height)]
    total[...] += jnp.dot(
        slab.reshape(total.shape[0], slab.shape[-1]),
        weights[tap],
        preferred_element_type=jnp.float32,
    )


def near_kernel(frames_ref, weight_ref, near_ref, shifted, weights, sems):
    f_dev, height = frames_ref.shape[:2]
    load = load_taps(weight_ref, weights, sems, 0)

    @pl.loop(0, f_dev)
    def _(slot):
        shift_into(shifted, frames_ref[slot], slot)

    near_ref[...] = jnp.zeros_like(near_ref)

    @pl.loop(0, weights.shape[0])
    def _(tap):
        add_tap(near_ref, shifted, weights, load, tap, 0, tap // 3, lax.rem(tap, 3), f_dev, height)


def lagged_kernel(
    length_ref, past_ref, frames_ref, weight_ref, latent_weight_ref, near_ref, section_ref,
    latent_ref, shifted, weights, total, sems,
):
    f_dev, height, width, channels = frames_ref.shape
    lags, cells = past_ref.shape[0], height * width
    load = load_taps(weight_ref, weights, sems, 9)

    @pl.loop(0, lags)
    def _(slot):
        shift_into(shifted, past_ref[slot], slot)

    @pl.loop(0, f_dev - 1)
    def _(slot):
        shift_into(shifted, frames_ref[slot], slot + lags)

    total[...] = jnp.zeros_like(total)

    @pl.loop(0, weights.shape[0])
    def _(tap):
        start = lags - 1 - tap // 9
        add_tap(
            total, shifted, weights, load, tap, start, lax.rem(tap // 3, 3), lax.rem(tap, 3),
            f_dev, height,
        )

    first = lax.axis_index("ctx") * f_dev

    @pl.loop(0, f_dev)
    def _(slot):
        video = jnp.where(first + slot < length_ref[0], 1.0, 0.0)
        rows = pl.ds(pl.multiple_of(slot * cells, cells), cells)
        value = (
            frames_ref[slot].astype(jnp.float32).reshape(cells, channels)
            + near_ref[rows]
            + video * total[rows]
        ).astype(jnp.bfloat16)
        section_ref[slot] = value.reshape(height, width, channels)
        latent_ref[rows] = jnp.dot(
            value, latent_weight_ref[...], preferred_element_type=jnp.float32
        ).astype(jnp.bfloat16)


def conv_section(frames, past, length, conv_weight, latent_weight):
    f_dev, height, width, channels = frames.shape
    lags = past.shape[0]
    cells = f_dev * height * width
    weight = conv_weight.reshape(-1, channels, channels)

    def scratch(slots, taps):
        return [
            pltpu.VMEM((3, slots, height + 2, width, channels), jnp.bfloat16),
            pltpu.VMEM((taps, channels, channels), jnp.bfloat16),
        ]

    def cost(taps):
        return pl.CostEstimate(
            flops=2 * cells * taps * channels * channels,
            bytes_accessed=2 * taps * channels * channels,
            transcendentals=0,
        )

    near = pl.pallas_call(
        near_kernel,
        out_shape=jax.ShapeDtypeStruct((cells, channels), jnp.float32),
        in_specs=[VMEM, HBM],
        out_specs=VMEM,
        scratch_shapes=[*scratch(f_dev, 9), pltpu.SemaphoreType.DMA((9,))],
        compiler_params=pltpu.CompilerParams(vmem_limit_bytes=24 << 20),
        cost_estimate=cost(9),
        name="near",
    )(frames, weight)
    return pl.pallas_call(
        lagged_kernel,
        out_shape=(
            jax.ShapeDtypeStruct(frames.shape, jnp.bfloat16),
            jax.ShapeDtypeStruct((cells, latent_weight.shape[1]), jnp.bfloat16),
        ),
        in_specs=[SMEM, VMEM, VMEM, HBM, VMEM, VMEM],
        out_specs=(VMEM, VMEM),
        scratch_shapes=[
            *scratch(f_dev + lags - 1, 9 * lags),
            pltpu.VMEM((cells, channels), jnp.float32),
            pltpu.SemaphoreType.DMA((9 * lags,)),
        ],
        compiler_params=pltpu.CompilerParams(vmem_limit_bytes=36 << 20),
        cost_estimate=cost(9 * lags),
        name="lagged",
    )(length, past, frames, weight, latent_weight, near)


def deal_kernel(stream_ref, *outs):
    n = len(outs)
    me = lax.axis_index("ctx")
    for k, out in enumerate(outs):
        out[...] = stream_ref[:, lax.rem(me + k, n)]


def deal(blocks):
    f_dev, n, pos, width = blocks.shape
    shape = jax.ShapeDtypeStruct((f_dev, pos, width), blocks.dtype)
    return pl.pallas_call(
        deal_kernel,
        out_shape=(shape,) * n,
        in_specs=[VMEM],
        out_specs=(VMEM,) * n,
        compiler_params=pltpu.CompilerParams(vmem_limit_bytes=10 << 20),
        cost_estimate=pl.CostEstimate(
            flops=blocks.size, bytes_accessed=4 * blocks.size, transcendentals=0
        ),
        name="deal",
    )(blocks)


def to_owners(blocks):
    n = blocks.shape[1]
    if n > 8:
        return None, [lax.all_to_all(blocks.transpose(1, 0, 2, 3), "ctx", 0, 0)]
    pieces = deal(blocks)
    near_first = sorted(range(n), key=lambda k: (min(k, n - k), -k))
    halves = [near_first[: n // 2], near_first[n // 2 :]]
    moved = []
    for turns in halves:
        rows = [
            lax.ppermute(pieces[k], "ctx", [(i, (i + k) % n) for i in range(n)])
            if k
            else pieces[0]
            for k in turns
        ]
        moved.append(jnp.stack(rows))
    return halves, moved


def norm_kernel(halves, groups, patch_size, patches_ref, embed_ref, gain_ref, *refs):
    parts, (out_ref, held, embedded, sems) = refs[:-4], refs[-4:]
    me, me_ctx = lax.axis_index("dp"), lax.axis_index("ctx")
    width = embed_ref.shape[1]
    n, f_dev, pos = held.shape[1:4]
    copies = []
    for spot, part in enumerate(parts):
        group = lax.bitwise_xor(me, spot % groups)
        if halves is None:
            copies.append((part, held.at[group]))
            continue
        for i, k in enumerate(halves[spot // groups]):
            copies.append((part.at[i], held.at[group, lax.rem(me_ctx - k + n, n)]))
    copies = [pltpu.make_async_copy(a, b, sems.at[i]) for i, (a, b) in enumerate(copies)]
    for copy in copies:
        copy.start()
    for copy in copies:
        copy.wait()
    block, batch = f_dev * pos, embedded.shape[0]

    @pl.loop(0, out_ref.shape[0] * n * block // batch)
    def _(b):
        rows = pl.ds(pl.multiple_of(b * batch, 16), batch)
        embedded[...] = jnp.dot(
            patches_ref[rows, :patch_size], embed_ref[...], preferred_element_type=jnp.float32
        )

        @pl.loop(0, batch // block)
        def _(i):
            spot = b * (batch // block) + i
            group, device = spot // n, lax.rem(spot, n)
            stream = held[group, device].astype(jnp.float32).reshape(block, width)
            value = embedded[pl.ds(pl.multiple_of(i * block, 8), block)] + stream
            scale = lax.rsqrt(jnp.mean(value * value, axis=-1, keepdims=True) + 1e-06)
            value = value * scale * gain_ref[...]
            out_ref[group, device] = value.reshape(f_dev, pos, width).astype(jnp.bfloat16)


def norm_rows(patches, embed_weight, norm_gain, halves, parts, groups, n):
    f_dev, pos, width = parts[0].shape[1:]
    rows = groups * n * f_dev * pos
    if pos % 8:
        order = jnp.arange(groups, dtype=jnp.int32) ^ lax.axis_index("dp")
        held = jnp.stack(parts)[order].reshape(rows, width)
        value = jnp.dot(
            patches[:, : embed_weight.shape[0]], embed_weight, preferred_element_type=jnp.float32
        ) + held.astype(jnp.float32)
        scale = lax.rsqrt(jnp.mean(value * value, axis=-1, keepdims=True) + 1e-06)
        return (value * scale * norm_gain).astype(jnp.bfloat16)
    return pl.pallas_call(
        functools.partial(norm_kernel, halves, groups, embed_weight.shape[0]),
        out_shape=jax.ShapeDtypeStruct((groups, n, f_dev, pos, width), jnp.bfloat16),
        in_specs=[VMEM] * 3 + [HBM] * len(parts),
        out_specs=VMEM,
        scratch_shapes=[
            pltpu.VMEM((groups, n, f_dev, pos, width), jnp.bfloat16),
            pltpu.VMEM((rows // (2 * groups), width), jnp.float32),
            pltpu.SemaphoreType.DMA((groups * n,)),
        ],
        compiler_params=pltpu.CompilerParams(vmem_limit_bytes=26 << 20),
        cost_estimate=pl.CostEstimate(
            flops=2 * rows * width * 512, bytes_accessed=4 * rows * width, transcendentals=0
        ),
        name="norm",
    )(patches, embed_weight, norm_gain[None], *parts).reshape(rows, width)


def qkv_kernel(count, spots, has_total, normed_ref, *refs):
    refs = list(refs)
    total_ref = refs.pop(0) if has_total else None
    sems, weight, out_ref = refs.pop(), refs.pop(), refs.pop()
    depth = weight.shape[1]
    firsts = piece_rows(count, depth)
    copies, used = [], 0
    for i, pieces in enumerate(spots):
        row = 0
        for _ in pieces:
            piece = refs[used]
            copies.append(
                pltpu.make_async_copy(
                    piece, weight.at[i, pl.ds(row, piece.shape[0])], sems.at[used]
                )
            )
            row += piece.shape[0]
            used += 1
    for copy in copies:
        copy.start()
    for copy in copies:
        copy.wait()
    rows = normed_ref.shape[0]
    tile = rows // 4 if rows % 64 == 0 else rows

    @pl.loop(0, rows // tile)
    def _(i):
        span = pl.ds(pl.multiple_of(i * tile, 16), tile)
        total = total_ref[span] if has_total else None
        for j, pieces in enumerate(spots):
            first = firsts[pieces[0]]
            if count:
                first = pl.multiple_of(first, 128)
            product = jnp.dot(
                normed_ref[span, pl.ds(first, depth)], weight[j], preferred_element_type=jnp.float32
            )
            total = product if total is None else total + product
        out_ref[span] = total.astype(out_ref.dtype)


def project(normed, pieces, count, spots, total, is_last):
    depth, columns = pieces[0].shape
    chosen = [pieces[i] for spot in spots for i in spot]
    first = [] if total is None else [total]
    dtype = jnp.bfloat16 if is_last else jnp.float32
    return pl.pallas_call(
        functools.partial(qkv_kernel, count, spots, total is not None),
        out_shape=jax.ShapeDtypeStruct((normed.shape[0], columns), dtype),
        in_specs=[VMEM] * (1 + len(first)) + [HBM] * len(chosen),
        out_specs=VMEM,
        scratch_shapes=[
            pltpu.VMEM((len(spots), depth, columns), jnp.bfloat16),
            pltpu.SemaphoreType.DMA((len(chosen),)),
        ],
        compiler_params=pltpu.CompilerParams(vmem_limit_bytes=32 << 20),
        cost_estimate=pl.CostEstimate(
            flops=2 * normed.shape[0] * len(spots) * depth * columns,
            bytes_accessed=2 * normed.size,
            transcendentals=0,
        ),
        name="qkv",
    )(normed, *first, *chosen)


def project_all(normed, pieces, count):
    if not count:
        return project(normed, pieces, count, ((0,),), None, True)
    last = len(pieces) - 2
    early = max(1, last - 2)
    stages = [tuple((i,) for i in range(early))]
    if early < last:
        stages.append(tuple((i,) for i in range(early, last)))
    stages.append(((last, last + 1),))
    total = None
    for s, spots in enumerate(stages):
        total = project(normed, pieces, count, spots, total, s == len(stages) - 1)
    return total


def attend(qkv, lengths):
    query, keys, values = (qkv[..., i * HD : (i + 1) * HD] for i in range(3))
    scores = jnp.einsum(
        "gtphd,gsphd->gphts", query, keys, preferred_element_type=jnp.float32
    ) * HD ** (-0.5)
    frame_ids = jnp.arange(qkv.shape[1], dtype=jnp.int32)
    video = frame_ids[None, :] < lengths[:, None]
    allowed = (
        video[:, :, None] & video[:, None, :] | (frame_ids[:, None] == frame_ids[None, :])[None]
    )
    scores = jnp.where(allowed[:, None, None], scores, -1e30)
    top = jnp.max(scores, axis=-1, keepdims=True)
    expo = jnp.exp(scores - top)
    probs = (expo / jnp.sum(expo, axis=-1, keepdims=True)).astype(jnp.bfloat16)
    return jnp.einsum(
        "gphts,gsphd->gtphd", probs, values, preferred_element_type=jnp.float32
    ).astype(jnp.bfloat16)


def body(
    frames, stream, video_frames, conv_weight, latent_weight, embed_weight, norm_gain, qkv_weight
):
    f_dev, height, width, _ = frames.shape[1:]
    tokens, width_model = stream.shape[2:]
    n, groups = lax.axis_size("ctx"), lax.axis_size("dp")
    pos = tokens // n
    heads = qkv_weight.shape[1] // (3 * HD)

    past = lax.ppermute(frames[0, f_dev - 2 :], "ctx", [(i, i + 1) for i in range(n - 1)])

    halves, moved = to_owners(stream[0].reshape(f_dev, n, pos, width_model))
    parts = []
    for value in moved:
        slots = {0: value}
        bit = groups // 2
        while bit:
            for j in sorted(slots):
                slots[j ^ bit] = flip(slots[j], "dp", bit)
            bit //= 2
        parts += [slots[j] for j in range(groups)]

    pieces = gather_ring(qkv_weight, "ctx")

    section, latent = conv_section(frames[0], past, video_frames, conv_weight, latent_weight)
    lat = latent.shape[1]
    patches = (
        latent.reshape(f_dev, height // 2, 2, width // 2, 2, lat)
        .transpose(0, 1, 3, 2, 4, 5)
        .reshape(f_dev, n, pos, 4 * lat)
        .transpose(1, 0, 2, 3)
    )
    length = jnp.broadcast_to(video_frames.astype(jnp.bfloat16), (*patches.shape[:-1], 1))
    patches = jnp.concatenate([patches, length], axis=-1)
    patches = jnp.broadcast_to(patches[None], (groups, *patches.shape)).reshape(
        groups * n, f_dev, pos, -1
    )
    patches = lax.all_to_all(patches, ("dp", "ctx"), 0, 0, tiled=True)
    rows = groups * n * f_dev * pos
    patches = patches.reshape(rows, -1)
    lengths = patches[:: rows // groups, -1].astype(jnp.int32)

    normed = norm_rows(patches, embed_weight, norm_gain, halves, parts, groups, n)
    qkv = project_all(normed, pieces, ring_size("ctx"))
    out = attend(qkv.reshape(groups, n * f_dev, pos, heads, 3 * HD), lengths)
    out = lax.all_to_all(
        out.reshape(groups * n, f_dev, pos, heads * HD), ("dp", "ctx"), 0, 0, tiled=True
    )
    out = out.reshape(groups, n, f_dev, pos, heads * HD).transpose(2, 1, 3, 0, 4)
    return section[None], out.reshape(1, f_dev, tokens, groups * heads * HD)


def solution(mesh):
    return jax.shard_map(
        body,
        mesh=mesh,
        in_specs=(
            P("dp", "ctx", None, None, None),
            P("dp", "ctx", None, None),
            P("dp"),
            P(),
            P(),
            P(),
            P(),
            P("ctx", "dp"),
        ),
        out_specs=(P("dp", "ctx", None, None, None), P("dp", "ctx", None, None)),
        check_vma=False,
    )
```

```python
import functools

import jax
import jax.numpy as jnp
from jax import lax
from jax.experimental import pallas as pl
from jax.experimental.pallas import tpu as pltpu
from jax.sharding import PartitionSpec as P

HD = 128
VMEM = pl.BlockSpec(memory_space=pltpu.VMEM)
HBM = pl.BlockSpec(memory_space=pltpu.HBM)
SMEM = pl.BlockSpec(memory_space=pltpu.SMEM)


def flip(value, axis, bit):
    count = lax.axis_size(axis)
    return lax.ppermute(value, axis, [(i, i ^ bit) for i in range(count)])


def ring_size(axis):
    count = lax.axis_size(axis)
    return count if count <= 8 and count % 2 == 0 else 0


def gather_ring(block, axis):
    count = ring_size(axis)
    if not count:
        return [lax.all_gather(block, axis, axis=0, tiled=True)]
    cycle = list(range(0, count, 2)) + list(range(count - 1, 0, -2))
    ahead = [(cycle[r], cycle[(r + 1) % count]) for r in range(count)]
    behind = [(b, a) for a, b in ahead]
    half = block.shape[0] // 2
    pieces = [block]
    ups = downs = (block[:half], block[half:])
    for _ in range(1, count // 2):
        moved = []
        for up, down in zip(ups, downs):
            moved.append((lax.ppermute(up, axis, ahead), lax.ppermute(down, axis, behind)))
        ups, downs = zip(*moved)
        pieces += [*ups, *downs]
    pieces.append(lax.ppermute(ups[0], axis, ahead))
    pieces.append(lax.ppermute(downs[1], axis, behind))
    return pieces


def piece_rows(count, rows):
    if not count:
        return [0]
    me = lax.axis_index("ctx")
    place = jnp.where(lax.rem(me, 2) == 0, me // 2, count - 1 - me // 2)

    def owner(shift):
        spot = lax.rem(place + shift + count, count)
        return jnp.where(spot < count // 2, 2 * spot, 2 * (count - 1 - spot) + 1) * rows

    first = [me * rows]
    for step in range(1, count // 2):
        first += [owner(-step)] * 2 + [owner(step)] * 2
    return first + [owner(count // 2)] * 2


def load_taps(weight_ref, weights, sems, first):
    def load(tap):
        return pltpu.make_async_copy(weight_ref.at[first + tap], weights.at[tap], sems.at[tap])

    for tap in range(weights.shape[0]):
        load(tap).start()
    return load


def shift_into(shifted, source, slot):
    height, width, channels = source.shape
    cells = height * width
    column = lax.rem(lax.broadcasted_iota(jnp.int32, (cells, channels), 0), width)
    edge = jnp.zeros((width, channels), jnp.bfloat16)
    act = jax.nn.silu(source.astype(jnp.float32)).reshape(cells, channels)
    left = jnp.where(column == 0, 0.0, pltpu.roll(act, 1, 0))
    right = jnp.where(column == width - 1, 0.0, pltpu.roll(act, cells - 1, 0))
    for col, value in enumerate((left, act, right)):
        shifted[col, slot, 0] = edge
        shifted[col, slot, height + 1] = edge
        shifted[col, slot, 1 : height + 1] = value.astype(jnp.bfloat16).reshape(source.shape)


def add_tap(total, shifted, weights, load, tap, start, row, col, f_dev, height):
    load(tap).wait()
    slab = shifted[col, pl.ds(start, f_dev), pl.ds(row, height)]
    total[...] += jnp.dot(
        slab.reshape(total.shape[0], slab.shape[-1]),
        weights[tap],
        preferred_element_type=jnp.float32,
    )


def near_kernel(frames_ref, weight_ref, near_ref, shifted, weights, sems):
    f_dev, height = frames_ref.shape[:2]
    load = load_taps(weight_ref, weights, sems, 0)

    @pl.loop(0, f_dev)
    def _(slot):
        shift_into(shifted, frames_ref[slot], slot)

    near_ref[...] = jnp.zeros_like(near_ref)

    @pl.loop(0, weights.shape[0])
    def _(tap):
        add_tap(near_ref, shifted, weights, load, tap, 0, tap // 3, lax.rem(tap, 3), f_dev, height)


def lagged_kernel(
    length_ref, past_ref, frames_ref, weight_ref, latent_weight_ref, near_ref, section_ref,
    latent_ref, shifted, weights, total, sems,
):
    f_dev, height, width, channels = frames_ref.shape
    lags, cells = past_ref.shape[0], height * width
    load = load_taps(weight_ref, weights, sems, 9)

    @pl.loop(0, lags)
    def _(slot):
        shift_into(shifted, past_ref[slot], slot)

    @pl.loop(0, f_dev - 1)
    def _(slot):
        shift_into(shifted, frames_ref[slot], slot + lags)

    total[...] = jnp.zeros_like(total)

    @pl.loop(0, weights.shape[0])
    def _(tap):
        start = lags - 1 - tap // 9
        add_tap(
            total, shifted, weights, load, tap, start, lax.rem(tap // 3, 3), lax.rem(tap, 3),
            f_dev, height,
        )

    first = lax.axis_index("ctx") * f_dev

    @pl.loop(0, f_dev)
    def _(slot):
        video = jnp.where(first + slot < length_ref[0], 1.0, 0.0)
        rows = pl.ds(pl.multiple_of(slot * cells, cells), cells)
        value = (
            frames_ref[slot].astype(jnp.float32).reshape(cells, channels)
            + near_ref[rows]
            + video * total[rows]
        ).astype(jnp.bfloat16)
        section_ref[slot] = value.reshape(height, width, channels)
        latent_ref[rows] = jnp.dot(
            value, latent_weight_ref[...], preferred_element_type=jnp.float32
        ).astype(jnp.bfloat16)


def conv_section(frames, past, length, conv_weight, latent_weight):
    f_dev, height, width, channels = frames.shape
    lags = past.shape[0]
    cells = f_dev * height * width
    weight = conv_weight.reshape(-1, channels, channels)

    def scratch(slots, taps):
        return [
            pltpu.VMEM((3, slots, height + 2, width, channels), jnp.bfloat16),
            pltpu.VMEM((taps, channels, channels), jnp.bfloat16),
        ]

    def cost(taps):
        return pl.CostEstimate(
            flops=2 * cells * taps * channels * channels,
            bytes_accessed=2 * taps * channels * channels,
            transcendentals=0,
        )

    near = pl.pallas_call(
        near_kernel,
        out_shape=jax.ShapeDtypeStruct((cells, channels), jnp.float32),
        in_specs=[VMEM, HBM],
        out_specs=VMEM,
        scratch_shapes=[*scratch(f_dev, 9), pltpu.SemaphoreType.DMA((9,))],
        compiler_params=pltpu.CompilerParams(vmem_limit_bytes=24 << 20),
        cost_estimate=cost(9),
        name="near",
    )(frames, weight)
    return pl.pallas_call(
        lagged_kernel,
        out_shape=(
            jax.ShapeDtypeStruct(frames.shape, jnp.bfloat16),
            jax.ShapeDtypeStruct((cells, latent_weight.shape[1]), jnp.bfloat16),
        ),
        in_specs=[SMEM, VMEM, VMEM, HBM, VMEM, VMEM],
        out_specs=(VMEM, VMEM),
        scratch_shapes=[
            *scratch(f_dev + lags - 1, 9 * lags),
            pltpu.VMEM((cells, channels), jnp.float32),
            pltpu.SemaphoreType.DMA((9 * lags,)),
        ],
        compiler_params=pltpu.CompilerParams(vmem_limit_bytes=36 << 20),
        cost_estimate=cost(9 * lags),
        name="lagged",
    )(length, past, frames, weight, latent_weight, near)


def deal_kernel(stream_ref, *outs):
    n = len(outs)
    me = lax.axis_index("ctx")
    for k, out in enumerate(outs):
        out[...] = stream_ref[:, lax.rem(me + k, n)]


def deal(blocks):
    f_dev, n, pos, width = blocks.shape
    shape = jax.ShapeDtypeStruct((f_dev, pos, width), blocks.dtype)
    return pl.pallas_call(
        deal_kernel,
        out_shape=(shape,) * n,
        in_specs=[VMEM],
        out_specs=(VMEM,) * n,
        compiler_params=pltpu.CompilerParams(vmem_limit_bytes=10 << 20),
        cost_estimate=pl.CostEstimate(
            flops=blocks.size, bytes_accessed=4 * blocks.size, transcendentals=0
        ),
        name="deal",
    )(blocks)


def to_owners(blocks):
    n = blocks.shape[1]
    if n > 8:
        return None, [lax.all_to_all(blocks.transpose(1, 0, 2, 3), "ctx", 0, 0)]
    pieces = deal(blocks)
    near_first = sorted(range(n), key=lambda k: (min(k, n - k), -k))
    halves = [near_first[: n // 2], near_first[n // 2 :]]
    moved = []
    for turns in halves:
        rows = [
            lax.ppermute(pieces[k], "ctx", [(i, (i + k) % n) for i in range(n)])
            if k
            else pieces[0]
            for k in turns
        ]
        moved.append(jnp.stack(rows))
    return halves, moved


def norm_kernel(halves, groups, patch_size, patches_ref, embed_ref, gain_ref, *refs):
    parts, (out_ref, held, embedded, sems) = refs[:-4], refs[-4:]
    me, me_ctx = lax.axis_index("dp"), lax.axis_index("ctx")
    width = embed_ref.shape[1]
    n, f_dev, pos = held.shape[1:4]
    copies = []
    for spot, part in enumerate(parts):
        group = lax.bitwise_xor(me, spot % groups)
        if halves is None:
            copies.append((part, held.at[group]))
            continue
        for i, k in enumerate(halves[spot // groups]):
            copies.append((part.at[i], held.at[group, lax.rem(me_ctx - k + n, n)]))
    copies = [pltpu.make_async_copy(a, b, sems.at[i]) for i, (a, b) in enumerate(copies)]
    for copy in copies:
        copy.start()
    for copy in copies:
        copy.wait()
    block, batch = f_dev * pos, embedded.shape[0]

    @pl.loop(0, out_ref.shape[0] * n * block // batch)
    def _(b):
        rows = pl.ds(pl.multiple_of(b * batch, 16), batch)
        embedded[...] = jnp.dot(
            patches_ref[rows, :patch_size], embed_ref[...], preferred_element_type=jnp.float32
        )

        @pl.loop(0, batch // block)
        def _(i):
            spot = b * (batch // block) + i
            group, device = spot // n, lax.rem(spot, n)
            stream = held[group, device].astype(jnp.float32).reshape(block, width)
            value = embedded[pl.ds(pl.multiple_of(i * block, 8), block)] + stream
            scale = lax.rsqrt(jnp.mean(value * value, axis=-1, keepdims=True) + 1e-06)
            value = value * scale * gain_ref[...]
            out_ref[group, device] = value.reshape(f_dev, pos, width).astype(jnp.bfloat16)


def norm_rows(patches, embed_weight, norm_gain, halves, parts, groups, n):
    f_dev, pos, width = parts[0].shape[1:]
    rows = groups * n * f_dev * pos
    if pos % 8:
        order = jnp.arange(groups, dtype=jnp.int32) ^ lax.axis_index("dp")
        held = jnp.stack(parts)[order].reshape(rows, width)
        value = jnp.dot(
            patches[:, : embed_weight.shape[0]], embed_weight, preferred_element_type=jnp.float32
        ) + held.astype(jnp.float32)
        scale = lax.rsqrt(jnp.mean(value * value, axis=-1, keepdims=True) + 1e-06)
        return (value * scale * norm_gain).astype(jnp.bfloat16)
    return pl.pallas_call(
        functools.partial(norm_kernel, halves, groups, embed_weight.shape[0]),
        out_shape=jax.ShapeDtypeStruct((groups, n, f_dev, pos, width), jnp.bfloat16),
        in_specs=[VMEM] * 3 + [HBM] * len(parts),
        out_specs=VMEM,
        scratch_shapes=[
            pltpu.VMEM((groups, n, f_dev, pos, width), jnp.bfloat16),
            pltpu.VMEM((rows // (2 * groups), width), jnp.float32),
            pltpu.SemaphoreType.DMA((groups * n,)),
        ],
        compiler_params=pltpu.CompilerParams(vmem_limit_bytes=26 << 20),
        cost_estimate=pl.CostEstimate(
            flops=2 * rows * width * 512, bytes_accessed=4 * rows * width, transcendentals=0
        ),
        name="norm",
    )(patches, embed_weight, norm_gain[None], *parts).reshape(rows, width)


def qkv_kernel(count, spots, has_total, normed_ref, *refs):
    refs = list(refs)
    total_ref = refs.pop(0) if has_total else None
    sems, weight, out_ref = refs.pop(), refs.pop(), refs.pop()
    depth = weight.shape[1]
    firsts = piece_rows(count, depth)
    copies, used = [], 0
    for i, pieces in enumerate(spots):
        row = 0
        for _ in pieces:
            piece = refs[used]
            copies.append(
                pltpu.make_async_copy(
                    piece, weight.at[i, pl.ds(row, piece.shape[0])], sems.at[used]
                )
            )
            row += piece.shape[0]
            used += 1
    for copy in copies:
        copy.start()
    for copy in copies:
        copy.wait()
    rows = normed_ref.shape[0]
    tile = rows // 4 if rows % 64 == 0 else rows

    @pl.loop(0, rows // tile)
    def _(i):
        span = pl.ds(pl.multiple_of(i * tile, 16), tile)
        total = total_ref[span] if has_total else None
        for j, pieces in enumerate(spots):
            first = firsts[pieces[0]]
            if count:
                first = pl.multiple_of(first, 128)
            product = jnp.dot(
                normed_ref[span, pl.ds(first, depth)], weight[j], preferred_element_type=jnp.float32
            )
            total = product if total is None else total + product
        out_ref[span] = total.astype(out_ref.dtype)


def project(normed, pieces, count, spots, total, is_last):
    depth, columns = pieces[0].shape
    chosen = [pieces[i] for spot in spots for i in spot]
    first = [] if total is None else [total]
    dtype = jnp.bfloat16 if is_last else jnp.float32
    return pl.pallas_call(
        functools.partial(qkv_kernel, count, spots, total is not None),
        out_shape=jax.ShapeDtypeStruct((normed.shape[0], columns), dtype),
        in_specs=[VMEM] * (1 + len(first)) + [HBM] * len(chosen),
        out_specs=VMEM,
        scratch_shapes=[
            pltpu.VMEM((len(spots), depth, columns), jnp.bfloat16),
            pltpu.SemaphoreType.DMA((len(chosen),)),
        ],
        compiler_params=pltpu.CompilerParams(vmem_limit_bytes=32 << 20),
        cost_estimate=pl.CostEstimate(
            flops=2 * normed.shape[0] * len(spots) * depth * columns,
            bytes_accessed=2 * normed.size,
            transcendentals=0,
        ),
        name="qkv",
    )(normed, *first, *chosen)


def project_all(normed, pieces, count):
    if not count:
        return project(normed, pieces, count, ((0,),), None, True)
    last = len(pieces) - 2
    early = max(1, last - 4)
    stages = [((0,), *((i, i + 1) for i in range(1, early, 2)))]
    if early < last:
        stages.append(tuple((i, i + 1) for i in range(early, last, 2)))
    stages.append(((last, last + 1),))
    total = None
    for s, spots in enumerate(stages):
        total = project(normed, pieces, count, spots, total, s == len(stages) - 1)
    return total


def attend(qkv, lengths):
    query, keys, values = (qkv[..., i * HD : (i + 1) * HD] for i in range(3))
    scores = jnp.einsum(
        "gtphd,gsphd->gphts", query, keys, preferred_element_type=jnp.float32
    ) * HD ** (-0.5)
    frame_ids = jnp.arange(qkv.shape[1], dtype=jnp.int32)
    video = frame_ids[None, :] < lengths[:, None]
    allowed = (
        video[:, :, None] & video[:, None, :] | (frame_ids[:, None] == frame_ids[None, :])[None]
    )
    scores = jnp.where(allowed[:, None, None], scores, -1e30)
    top = jnp.max(scores, axis=-1, keepdims=True)
    expo = jnp.exp(scores - top)
    probs = (expo / jnp.sum(expo, axis=-1, keepdims=True)).astype(jnp.bfloat16)
    return jnp.einsum(
        "gphts,gsphd->gtphd", probs, values, preferred_element_type=jnp.float32
    ).astype(jnp.bfloat16)


def body(
    frames, stream, video_frames, conv_weight, latent_weight, embed_weight, norm_gain, qkv_weight
):
    f_dev, height, width, _ = frames.shape[1:]
    tokens, width_model = stream.shape[2:]
    n, groups = lax.axis_size("ctx"), lax.axis_size("dp")
    pos = tokens // n
    heads = qkv_weight.shape[1] // (3 * HD)

    past = lax.ppermute(frames[0, f_dev - 2 :], "ctx", [(i, i + 1) for i in range(n - 1)])

    halves, moved = to_owners(stream[0].reshape(f_dev, n, pos, width_model))
    parts = []
    for value in moved:
        slots = {0: value}
        bit = groups // 2
        while bit:
            for j in sorted(slots):
                slots[j ^ bit] = flip(slots[j], "dp", bit)
            bit //= 2
        parts += [slots[j] for j in range(groups)]

    pieces = gather_ring(qkv_weight, "ctx")

    section, latent = conv_section(frames[0], past, video_frames, conv_weight, latent_weight)
    lat = latent.shape[1]
    patches = (
        latent.reshape(f_dev, height // 2, 2, width // 2, 2, lat)
        .transpose(0, 1, 3, 2, 4, 5)
        .reshape(f_dev, n, pos, 4 * lat)
        .transpose(1, 0, 2, 3)
    )
    length = jnp.broadcast_to(video_frames.astype(jnp.bfloat16), (*patches.shape[:-1], 1))
    patches = jnp.concatenate([patches, length], axis=-1)
    patches = jnp.broadcast_to(patches[None], (groups, *patches.shape)).reshape(
        groups * n, f_dev, pos, -1
    )
    patches = lax.all_to_all(patches, ("dp", "ctx"), 0, 0, tiled=True)
    rows = groups * n * f_dev * pos
    patches = patches.reshape(rows, -1)
    lengths = patches[:: rows // groups, -1].astype(jnp.int32)

    normed = norm_rows(patches, embed_weight, norm_gain, halves, parts, groups, n)
    qkv = project_all(normed, pieces, ring_size("ctx"))
    out = attend(qkv.reshape(groups, n * f_dev, pos, heads, 3 * HD), lengths)
    out = lax.all_to_all(
        out.reshape(groups * n, f_dev, pos, heads * HD), ("dp", "ctx"), 0, 0, tiled=True
    )
    out = out.reshape(groups, n, f_dev, pos, heads * HD).transpose(2, 1, 3, 0, 4)
    return section[None], out.reshape(1, f_dev, tokens, groups * heads * HD)


def solution(mesh):
    return jax.shard_map(
        body,
        mesh=mesh,
        in_specs=(
            P("dp", "ctx", None, None, None),
            P("dp", "ctx", None, None),
            P("dp"),
            P(),
            P(),
            P(),
            P(),
            P("ctx", "dp"),
        ),
        out_specs=(P("dp", "ctx", None, None, None), P("dp", "ctx", None, None)),
        check_vma=False,
    )
```

```python
import functools

import jax
import jax.numpy as jnp
from jax import lax
from jax.experimental import pallas as pl
from jax.experimental.pallas import tpu as pltpu
from jax.sharding import PartitionSpec as P

HD = 128
VMEM = pl.BlockSpec(memory_space=pltpu.VMEM)
HBM = pl.BlockSpec(memory_space=pltpu.HBM)
SMEM = pl.BlockSpec(memory_space=pltpu.SMEM)


def flip(value, axis, bit):
    count = lax.axis_size(axis)
    return lax.ppermute(value, axis, [(i, i ^ bit) for i in range(count)])


def ring_size(axis):
    count = lax.axis_size(axis)
    return count if count <= 8 and count % 2 == 0 else 0


def gather_ring(block, axis):
    count = ring_size(axis)
    if not count:
        return [lax.all_gather(block, axis, axis=0, tiled=True)]
    cycle = list(range(0, count, 2)) + list(range(count - 1, 0, -2))
    ahead = [(cycle[r], cycle[(r + 1) % count]) for r in range(count)]
    behind = [(b, a) for a, b in ahead]
    pieces = [block]
    up = down = block
    for _ in range(1, count // 2):
        up = lax.ppermute(up, axis, ahead)
        down = lax.ppermute(down, axis, behind)
        pieces += [up, down]
    half = block.shape[0] // 2
    pieces.append(lax.ppermute(up[:half], axis, ahead))
    pieces.append(lax.ppermute(down[half:], axis, behind))
    return pieces


def piece_rows(count, rows):
    if not count:
        return [0]
    me = lax.axis_index("ctx")
    place = jnp.where(lax.rem(me, 2) == 0, me // 2, count - 1 - me // 2)

    def owner(shift):
        spot = lax.rem(place + shift + count, count)
        return jnp.where(spot < count // 2, 2 * spot, 2 * (count - 1 - spot) + 1) * rows

    first = [me * rows]
    for step in range(1, count // 2):
        first += [owner(-step), owner(step)]
    far = owner(count // 2)
    return first + [far, far + rows // 2]


def load_taps(weight_ref, weights, sems, first):
    def load(tap):
        return pltpu.make_async_copy(weight_ref.at[first + tap], weights.at[tap], sems.at[tap])

    for tap in range(weights.shape[0]):
        load(tap).start()
    return load


def shift_into(shifted, source, slot):
    height, width, channels = source.shape
    cells = height * width
    column = lax.rem(lax.broadcasted_iota(jnp.int32, (cells, channels), 0), width)
    edge = jnp.zeros((width, channels), jnp.bfloat16)
    act = jax.nn.silu(source.astype(jnp.float32)).reshape(cells, channels)
    left = jnp.where(column == 0, 0.0, pltpu.roll(act, 1, 0))
    right = jnp.where(column == width - 1, 0.0, pltpu.roll(act, cells - 1, 0))
    for col, value in enumerate((left, act, right)):
        shifted[col, slot, 0] = edge
        shifted[col, slot, height + 1] = edge
        shifted[col, slot, 1 : height + 1] = value.astype(jnp.bfloat16).reshape(source.shape)


def add_tap(total, shifted, weights, load, tap, start, row, col, f_dev, height):
    load(tap).wait()
    slab = shifted[col, pl.ds(start, f_dev), pl.ds(row, height)]
    total[...] += jnp.dot(
        slab.reshape(total.shape[0], slab.shape[-1]),
        weights[tap],
        preferred_element_type=jnp.float32,
    )


def near_kernel(frames_ref, weight_ref, near_ref, shifted, weights, sems):
    f_dev, height = frames_ref.shape[:2]
    load = load_taps(weight_ref, weights, sems, 0)

    @pl.loop(0, f_dev)
    def _(slot):
        shift_into(shifted, frames_ref[slot], slot)

    near_ref[...] = jnp.zeros_like(near_ref)

    @pl.loop(0, weights.shape[0])
    def _(tap):
        add_tap(near_ref, shifted, weights, load, tap, 0, tap // 3, lax.rem(tap, 3), f_dev, height)


def lagged_kernel(
    length_ref, past_ref, frames_ref, weight_ref, latent_weight_ref, near_ref, section_ref,
    latent_ref, shifted, weights, total, sems,
):
    f_dev, height, width, channels = frames_ref.shape
    lags, cells = past_ref.shape[0], height * width
    load = load_taps(weight_ref, weights, sems, 9)

    @pl.loop(0, lags)
    def _(slot):
        shift_into(shifted, past_ref[slot], slot)

    @pl.loop(0, f_dev - 1)
    def _(slot):
        shift_into(shifted, frames_ref[slot], slot + lags)

    total[...] = jnp.zeros_like(total)

    @pl.loop(0, weights.shape[0])
    def _(tap):
        start = lags - 1 - tap // 9
        add_tap(
            total, shifted, weights, load, tap, start, lax.rem(tap // 3, 3), lax.rem(tap, 3),
            f_dev, height,
        )

    first = lax.axis_index("ctx") * f_dev

    @pl.loop(0, f_dev)
    def _(slot):
        video = jnp.where(first + slot < length_ref[0], 1.0, 0.0)
        rows = pl.ds(pl.multiple_of(slot * cells, cells), cells)
        value = (
            frames_ref[slot].astype(jnp.float32).reshape(cells, channels)
            + near_ref[rows]
            + video * total[rows]
        ).astype(jnp.bfloat16)
        section_ref[slot] = value.reshape(height, width, channels)
        latent_ref[rows] = jnp.dot(
            value, latent_weight_ref[...], preferred_element_type=jnp.float32
        ).astype(jnp.bfloat16)


def conv_section(frames, past, length, conv_weight, latent_weight):
    f_dev, height, width, channels = frames.shape
    lags = past.shape[0]
    cells = f_dev * height * width
    weight = conv_weight.reshape(-1, channels, channels)

    def scratch(slots, taps):
        return [
            pltpu.VMEM((3, slots, height + 2, width, channels), jnp.bfloat16),
            pltpu.VMEM((taps, channels, channels), jnp.bfloat16),
        ]

    def cost(taps):
        return pl.CostEstimate(
            flops=2 * cells * taps * channels * channels,
            bytes_accessed=2 * taps * channels * channels,
            transcendentals=0,
        )

    near = pl.pallas_call(
        near_kernel,
        out_shape=jax.ShapeDtypeStruct((cells, channels), jnp.float32),
        in_specs=[VMEM, HBM],
        out_specs=VMEM,
        scratch_shapes=[*scratch(f_dev, 9), pltpu.SemaphoreType.DMA((9,))],
        compiler_params=pltpu.CompilerParams(vmem_limit_bytes=24 << 20),
        cost_estimate=cost(9),
        name="near",
    )(frames, weight)
    return pl.pallas_call(
        lagged_kernel,
        out_shape=(
            jax.ShapeDtypeStruct(frames.shape, jnp.bfloat16),
            jax.ShapeDtypeStruct((cells, latent_weight.shape[1]), jnp.bfloat16),
        ),
        in_specs=[SMEM, VMEM, VMEM, HBM, VMEM, VMEM],
        out_specs=(VMEM, VMEM),
        scratch_shapes=[
            *scratch(f_dev + lags - 1, 9 * lags),
            pltpu.VMEM((cells, channels), jnp.float32),
            pltpu.SemaphoreType.DMA((9 * lags,)),
        ],
        compiler_params=pltpu.CompilerParams(vmem_limit_bytes=36 << 20),
        cost_estimate=cost(9 * lags),
        name="lagged",
    )(length, past, frames, weight, latent_weight, near)


def deal_kernel(stream_ref, *outs):
    n = len(outs)
    me = lax.axis_index("ctx")
    for k, out in enumerate(outs):
        out[...] = stream_ref[:, lax.rem(me + k, n)]


def deal(blocks):
    f_dev, n, pos, width = blocks.shape
    shape = jax.ShapeDtypeStruct((f_dev, pos, width), blocks.dtype)
    return pl.pallas_call(
        deal_kernel,
        out_shape=(shape,) * n,
        in_specs=[VMEM],
        out_specs=(VMEM,) * n,
        compiler_params=pltpu.CompilerParams(vmem_limit_bytes=10 << 20),
        cost_estimate=pl.CostEstimate(
            flops=blocks.size, bytes_accessed=4 * blocks.size, transcendentals=0
        ),
        name="deal",
    )(blocks)


def to_owners(blocks):
    n = blocks.shape[1]
    if n > 8:
        return None, [lax.all_to_all(blocks.transpose(1, 0, 2, 3), "ctx", 0, 0)]
    pieces = deal(blocks)
    near_first = sorted(range(n), key=lambda k: (min(k, n - k), -k))
    halves = [near_first[: n // 2], near_first[n // 2 :]]
    moved = []
    for turns in halves:
        rows = [
            lax.ppermute(pieces[k], "ctx", [(i, (i + k) % n) for i in range(n)])
            if k
            else pieces[0]
            for k in turns
        ]
        moved.append(jnp.stack(rows))
    return halves, moved


def norm_kernel(halves, groups, patch_size, patches_ref, embed_ref, gain_ref, *refs):
    parts, (out_ref, held, embedded, sems) = refs[:-4], refs[-4:]
    me, me_ctx = lax.axis_index("dp"), lax.axis_index("ctx")
    width = embed_ref.shape[1]
    n, f_dev, pos = held.shape[1:4]
    copies = []
    for spot, part in enumerate(parts):
        group = lax.bitwise_xor(me, spot % groups)
        if halves is None:
            copies.append((spot % groups, part, held.at[group]))
            continue
        for i, k in enumerate(halves[spot // groups]):
            place = held.at[group, lax.rem(me_ctx - k + n, n)]
            copies.append((spot % groups, part.at[i], place))
    copies.sort(key=lambda entry: entry[0])
    copies = [
        (slot, pltpu.make_async_copy(a, b, sems.at[i])) for i, (slot, a, b) in enumerate(copies)
    ]
    for _, copy in copies:
        copy.start()
    block, batch = f_dev * pos, embedded.shape[0]
    batches = n * block // batch
    for slot in range(groups):
        group = lax.bitwise_xor(me, slot)
        for owner, copy in copies:
            if owner == slot:
                copy.wait()

        @pl.loop(0, batches)
        def _(b, group=group):
            rows = pl.ds(pl.multiple_of((group * batches + b) * batch, 16), batch)
            embedded[...] = jnp.dot(
                patches_ref[rows, :patch_size], embed_ref[...], preferred_element_type=jnp.float32
            )

            @pl.loop(0, batch // block)
            def _(i):
                device = b * (batch // block) + i
                stream = held[group, device].astype(jnp.float32).reshape(block, width)
                value = embedded[pl.ds(pl.multiple_of(i * block, 8), block)] + stream
                scale = lax.rsqrt(jnp.mean(value * value, axis=-1, keepdims=True) + 1e-06)
                value = value * scale * gain_ref[...]
                out_ref[group, device] = value.reshape(f_dev, pos, width).astype(jnp.bfloat16)


def norm_rows(patches, embed_weight, norm_gain, halves, parts, groups, n):
    f_dev, pos, width = parts[0].shape[1:]
    rows = groups * n * f_dev * pos
    if pos % 8:
        order = jnp.arange(groups, dtype=jnp.int32) ^ lax.axis_index("dp")
        held = jnp.stack(parts)[order].reshape(rows, width)
        value = jnp.dot(
            patches[:, : embed_weight.shape[0]], embed_weight, preferred_element_type=jnp.float32
        ) + held.astype(jnp.float32)
        scale = lax.rsqrt(jnp.mean(value * value, axis=-1, keepdims=True) + 1e-06)
        return (value * scale * norm_gain).astype(jnp.bfloat16)
    return pl.pallas_call(
        functools.partial(norm_kernel, halves, groups, embed_weight.shape[0]),
        out_shape=jax.ShapeDtypeStruct((groups, n, f_dev, pos, width), jnp.bfloat16),
        in_specs=[VMEM] * 3 + [HBM] * len(parts),
        out_specs=VMEM,
        scratch_shapes=[
            pltpu.VMEM((groups, n, f_dev, pos, width), jnp.bfloat16),
            pltpu.VMEM((rows // (2 * groups), width), jnp.float32),
            pltpu.SemaphoreType.DMA((groups * n,)),
        ],
        compiler_params=pltpu.CompilerParams(vmem_limit_bytes=26 << 20),
        cost_estimate=pl.CostEstimate(
            flops=2 * rows * width * 512, bytes_accessed=4 * rows * width, transcendentals=0
        ),
        name="norm",
    )(patches, embed_weight, norm_gain[None], *parts).reshape(rows, width)


def qkv_kernel(count, spots, has_total, normed_ref, *refs):
    refs = list(refs)
    total_ref = refs.pop(0) if has_total else None
    sems, weight, out_ref = refs.pop(), refs.pop(), refs.pop()
    depth = weight.shape[0] // len(spots)
    firsts = piece_rows(count, depth)
    copies, used = [], 0
    for i, pieces in enumerate(spots):
        row = i * depth
        for _ in pieces:
            piece = refs[used]
            copies.append(
                pltpu.make_async_copy(
                    piece, weight.at[pl.ds(row, piece.shape[0])], sems.at[used]
                )
            )
            row += piece.shape[0]
            used += 1
    for copy in copies:
        copy.start()
    for copy in copies:
        copy.wait()
    rows = normed_ref.shape[0]
    tile = rows // 4 if rows % 64 == 0 else rows

    @pl.loop(0, rows // tile)
    def _(i):
        span = pl.ds(pl.multiple_of(i * tile, 16), tile)
        blocks = []
        for pieces in spots:
            first = firsts[pieces[0]]
            if count:
                first = pl.multiple_of(first, 128)
            blocks.append(normed_ref[span, pl.ds(first, depth)])
        total = jnp.dot(
            jnp.concatenate(blocks, axis=1), weight[...], preferred_element_type=jnp.float32
        )
        if has_total:
            total = total_ref[span] + total
        out_ref[span] = total.astype(out_ref.dtype)


def project(normed, pieces, count, spots, total, is_last):
    depth, columns = pieces[0].shape
    chosen = [pieces[i] for spot in spots for i in spot]
    first = [] if total is None else [total]
    dtype = jnp.bfloat16 if is_last else jnp.float32
    return pl.pallas_call(
        functools.partial(qkv_kernel, count, spots, total is not None),
        out_shape=jax.ShapeDtypeStruct((normed.shape[0], columns), dtype),
        in_specs=[VMEM] * (1 + len(first)) + [HBM] * len(chosen),
        out_specs=VMEM,
        scratch_shapes=[
            pltpu.VMEM((len(spots) * depth, columns), jnp.bfloat16),
            pltpu.SemaphoreType.DMA((len(chosen),)),
        ],
        compiler_params=pltpu.CompilerParams(vmem_limit_bytes=32 << 20),
        cost_estimate=pl.CostEstimate(
            flops=2 * normed.shape[0] * len(spots) * depth * columns,
            bytes_accessed=2 * normed.size,
            transcendentals=0,
        ),
        name="qkv",
    )(normed, *first, *chosen)


def project_all(normed, pieces, count):
    if not count:
        return project(normed, pieces, count, ((0,),), None, True)
    last = len(pieces) - 2
    early = max(1, last - 2)
    stages = [tuple((i,) for i in range(early))]
    if early < last:
        stages.append(tuple((i,) for i in range(early, last)))
    stages.append(((last, last + 1),))
    total = None
    for s, spots in enumerate(stages):
        total = project(normed, pieces, count, spots, total, s == len(stages) - 1)
    return total


def attend(qkv, lengths):
    query, keys, values = (qkv[..., i * HD : (i + 1) * HD] for i in range(3))
    scores = jnp.einsum(
        "gtphd,gsphd->gphts", query, keys, preferred_element_type=jnp.float32
    ) * HD ** (-0.5)
    frame_ids = jnp.arange(qkv.shape[1], dtype=jnp.int32)
    video = frame_ids[None, :] < lengths[:, None]
    allowed = (
        video[:, :, None] & video[:, None, :] | (frame_ids[:, None] == frame_ids[None, :])[None]
    )
    scores = jnp.where(allowed[:, None, None], scores, -1e30)
    top = jnp.max(scores, axis=-1, keepdims=True)
    expo = jnp.exp(scores - top)
    probs = (expo / jnp.sum(expo, axis=-1, keepdims=True)).astype(jnp.bfloat16)
    return jnp.einsum(
        "gphts,gsphd->gtphd", probs, values, preferred_element_type=jnp.float32
    ).astype(jnp.bfloat16)


def body(
    frames, stream, video_frames, conv_weight, latent_weight, embed_weight, norm_gain, qkv_weight
):
    f_dev, height, width, _ = frames.shape[1:]
    tokens, width_model = stream.shape[2:]
    n, groups = lax.axis_size("ctx"), lax.axis_size("dp")
    pos = tokens // n
    heads = qkv_weight.shape[1] // (3 * HD)

    past = lax.ppermute(frames[0, f_dev - 2 :], "ctx", [(i, i + 1) for i in range(n - 1)])

    halves, moved = to_owners(stream[0].reshape(f_dev, n, pos, width_model))
    parts = []
    for value in moved:
        slots = {0: value}
        bit = groups // 2
        while bit:
            for j in sorted(slots):
                slots[j ^ bit] = flip(slots[j], "dp", bit)
            bit //= 2
        parts += [slots[j] for j in range(groups)]

    pieces = gather_ring(qkv_weight, "ctx")

    section, latent = conv_section(frames[0], past, video_frames, conv_weight, latent_weight)
    lat = latent.shape[1]
    patches = (
        latent.reshape(f_dev, height // 2, 2, width // 2, 2, lat)
        .transpose(0, 1, 3, 2, 4, 5)
        .reshape(f_dev, n, pos, 4 * lat)
        .transpose(1, 0, 2, 3)
    )
    length = jnp.broadcast_to(video_frames.astype(jnp.bfloat16), (*patches.shape[:-1], 1))
    patches = jnp.concatenate([patches, length], axis=-1)
    patches = jnp.broadcast_to(patches[None], (groups, *patches.shape)).reshape(
        groups * n, f_dev, pos, -1
    )
    patches = lax.all_to_all(patches, ("dp", "ctx"), 0, 0, tiled=True)
    rows = groups * n * f_dev * pos
    patches = patches.reshape(rows, -1)
    lengths = patches[:: rows // groups, -1].astype(jnp.int32)

    normed = norm_rows(patches, embed_weight, norm_gain, halves, parts, groups, n)
    qkv = project_all(normed, pieces, ring_size("ctx"))
    out = attend(qkv.reshape(groups, n * f_dev, pos, heads, 3 * HD), lengths)
    out = lax.all_to_all(
        out.reshape(groups * n, f_dev, pos, heads * HD), ("dp", "ctx"), 0, 0, tiled=True
    )
    out = out.reshape(groups, n, f_dev, pos, heads * HD).transpose(2, 1, 3, 0, 4)
    return section[None], out.reshape(1, f_dev, tokens, groups * heads * HD)


def solution(mesh):
    return jax.shard_map(
        body,
        mesh=mesh,
        in_specs=(
            P("dp", "ctx", None, None, None),
            P("dp", "ctx", None, None),
            P("dp"),
            P(),
            P(),
            P(),
            P(),
            P("ctx", "dp"),
        ),
        out_specs=(P("dp", "ctx", None, None, None), P("dp", "ctx", None, None)),
        check_vma=False,
    )
```
